128 devices in a mesh: gx: 8 (over y_lo, x), gy: 8 (over z, core), gz: 2 (over y_hi).
Axes of the slice: x: 4, y: 4 (y_hi: 2, y_lo: 2; y = y_hi * 2 + y_lo), z: 4, core: 2. Of those that a mesh axis runs over, the one named last changes fastest.
Arguments:
- blocks: int32 [131072, 4], P(('gx', 'gy', 'gz')), may hold values from 0 to 15, as said below
- coefficients: bfloat16 [131072, 4, 128], P(('gx', 'gy', 'gz')), may hold values from -80 to 80
- residuals: float32 [131072], P(('gx', 'gy', 'gz')), may hold values from -3000 to 3000
Outputs:
- factor: float32 [8, 2, 128, 8, 2, 128], P('gx', None, None, 'gy')
- solution: float32 [16, 128], replicated
The draws below stay inside these ranges and needn't reach their ends.
Inputs may be any that keep to these rules, and one draw needn't show every extreme that they name: Each row names 4 different blocks.
All inputs are finite; a program needn't handle non-finite values.
Results may differ from the reference program's by a relative error of at most 0.0003.
Values sent between devices are 32-bit elements; how exact they have to be, the bound alone decides.
No kernel may reach another device: no remote copies, remote signals or barrier semaphores. Data moves between devices by JAX's collectives and lax.ppermute only.
A program may use at most 128 MiB of HBM per device.

```python
import math
import jax
import jax.numpy as jnp
from jax import lax

G = 2048
BS = 128
SLOTS = 4
OBS = 131072
N_GX = 8
N_GY = 8


def pick_blocks(key):
    nblock = G // BS
    base = jax.random.fold_in(key, 11)
    scores = jax.random.randint(base, (OBS, nblock), 0, 1 << 20) * nblock + jnp.arange(nblock, dtype=jnp.int32)[None, :]
    chosen = lax.top_k(scores, SLOTS)[1]
    return chosen.astype(jnp.int32)


def make_coefficients(key):
    base = jax.random.fold_in(key, 23)
    noise = jnp.clip(jax.random.normal(jax.random.fold_in(base, 1), (OBS, SLOTS, BS), jnp.float32), -6.0, 6.0)
    mixing = jax.random.normal(jax.random.fold_in(base, 3), (BS, BS), jnp.float32) / math.sqrt(BS)
    neighbour = jnp.roll(noise, -1, axis=1)
    coupled = noise + 0.35 * jnp.einsum('osx,xy->osy', neighbour, mixing)
    return jnp.clip(coupled, -80.0, 80.0)


def draw_blocks(key, part):
    return pick_blocks(key)


def draw_coefficients(key, part):
    return make_coefficients(key).astype(jnp.bfloat16)


def draw_residuals(key, part):
    coef = make_coefficients(key)
    chosen = pick_blocks(key)
    truth = jax.random.normal(jax.random.fold_in(key, 37), (G // BS, BS), jnp.float32)
    picked = truth[chosen]
    noise = jax.random.normal(jax.random.fold_in(key, 41), (OBS,), jnp.float32)
    values = jnp.sum(coef * picked, axis=(1, 2)) + noise
    return jnp.clip(values, -3000.0, 3000.0)


def setup_inputs(seed: int = 0) -> dict:
    key_list = jax.random.split(jax.random.key(seed), 4)
    blocks = draw_blocks(jax.random.fold_in(key_list[3], 71), 0)
    coefficients = draw_coefficients(jax.random.fold_in(key_list[3], 71), 0)
    residuals = draw_residuals(jax.random.fold_in(key_list[3], 71), 0)
    return {"blocks": blocks, "coefficients": coefficients, "residuals": residuals}


def reference(blocks, coefficients, residuals):
    total = blocks.shape[0]
    nblock = G // BS
    per_dev = nblock // N_GX
    group = math.gcd(total, 4096)
    count = total // group
    labels = jnp.arange(nblock, dtype=jnp.int32)

    def accumulate(carry, index):
        start = (index * group).astype(jnp.int32)
        picked = lax.dynamic_slice_in_dim(blocks, start, group, 0)
        coef = lax.dynamic_slice_in_dim(coefficients, start, group, 0).astype(jnp.float32)
        resid = lax.dynamic_slice_in_dim(residuals, start, group, 0)
        placed = (picked[:, :, None] == labels[None, None, :]).astype(jnp.float32)
        design = jnp.einsum('osa,osx->oax', placed, coef, precision=lax.Precision.HIGHEST).reshape(group, G)
        normal = carry[0] + jnp.dot(design.T.astype(jnp.float32), design.astype(jnp.float32), precision=lax.Precision.HIGHEST, preferred_element_type=jnp.float32)
        rhs = carry[1] + jnp.dot(resid.astype(jnp.float32), design.astype(jnp.float32), precision=lax.Precision.HIGHEST, preferred_element_type=jnp.float32)
        return ((normal, rhs), None)
    start_state = (jnp.zeros((G, G), jnp.float32), jnp.zeros((G,), jnp.float32))
    (normal, rhs), _ = lax.scan(accumulate, start_state, jnp.arange(count, dtype=jnp.int32))
    normal = normal / total
    rhs = rhs / total
    lower = jnp.linalg.cholesky(normal)
    middle = jax.scipy.linalg.solve_triangular(lower, rhs, lower=True)
    answer = jax.scipy.linalg.solve_triangular(lower.T, middle, lower=False)
    factor = lower.reshape(per_dev, N_GX, BS, per_dev, N_GY, BS).transpose(1, 0, 2, 4, 3, 5)
    return (factor, answer.reshape(nblock, BS))
```

```python
import jax
import jax.numpy as jnp
from jax import lax
from jax.experimental import pallas as pl
from jax.experimental.pallas import tpu as pltpu
from jax.sharding import PartitionSpec as P

G = 2048
BS = 128
W = 256
NB = G // W
NP = NB * (NB + 1) // 2
ROWS = NP * W + NB
ALL = ("gx", "gy", "gz")
F32 = jnp.float32
BF16 = jnp.bfloat16
VMEM_LIMIT = 60000 * 1024


def tri(i, j):
    return j * NB - (j * (j - 1)) // 2 + (i - j)


def nt(a, b):
    return lax.dot_general(a, b, (((1,), (1,)), ((), ())), preferred_element_type=F32)


def nn(a, b):
    return lax.dot_general(a, b, (((1,), (0,)), ((), ())), preferred_element_type=F32)


def split(x):
    hi = x.astype(BF16)
    return hi, (x - hi.astype(F32)).astype(BF16)


def three(dot, a, b):
    return dot(a[0], b[0]) + (dot(a[1], b[0]) + dot(a[0], b[1]))


def gram_kernel(blocks_ref, resid_ref, coef_ref, out_ref, c32, ct, dt):
    obs = blocks_ref.shape[1]
    slots = blocks_ref.shape[0]
    scale = 2.0**-17
    c32[...] = coef_ref[...].astype(F32)
    for s in range(slots):
        for h in range(obs // 128):
            ct[s, :, pl.ds(h * 128, 128)] = c32[pl.ds(h * 128 * slots + s, 128, stride=slots), :].T

    def place(b, carry):
        for h in range(obs // 128):
            lanes = pl.ds(h * 128, 128)
            picks = [
                jnp.broadcast_to(blocks_ref[s : s + 1, lanes], (BS, 128)) == b for s in range(slots)
            ]
            d = jnp.zeros((BS, 128), F32)
            for s in range(slots):
                d = jnp.where(picks[s], ct[s, :, lanes], d)
            dt[pl.ds(pl.multiple_of(b * BS, BS), BS), lanes] = d.astype(BF16)
        return carry

    lax.fori_loop(0, G // BS, place, 0)
    r = resid_ref[...]
    r0 = r.astype(BF16)
    left = r - r0.astype(F32)
    r1 = left.astype(BF16)
    r2 = (left - r1.astype(F32)).astype(BF16)
    sub = lax.broadcasted_iota(jnp.int32, (8, obs), 0)
    parts = jnp.where(sub == 0, r0.astype(F32), jnp.where(sub == 1, r1.astype(F32), jnp.where(sub == 2, r2.astype(F32), 0.0)))
    parts = parts.astype(BF16)

    for j in range(NB):
        dj = dt[pl.ds(j * W, W), :]
        sums = nt(parts, dj) * scale
        out_ref[pl.ds(NP * W + j, 1), :] = sums[0:1] + (sums[1:2] + sums[2:3])

        def row(i, carry):
            di = dt[pl.ds(pl.multiple_of(i * W, W), W), :]
            at = pl.multiple_of(tri(i, j) * W, W)
            out_ref[pl.ds(at, W), :] = nt(di, dt[pl.ds(j * W, W), :]) * scale
            return carry

        lax.fori_loop(j, NB, row, 0)


def gram(blocks, coefficients, residuals):
    obs, slots, width = coefficients.shape
    return pl.pallas_call(
        gram_kernel,
        out_shape=jax.ShapeDtypeStruct((ROWS, W), F32),
        scratch_shapes=[
            pltpu.VMEM((obs * slots, width), F32),
            pltpu.VMEM((slots, width, obs), F32),
            pltpu.VMEM((G, obs), BF16),
        ],
        compiler_params=pltpu.CompilerParams(vmem_limit_bytes=VMEM_LIMIT),
    )(blocks.T, residuals.reshape(1, obs), coefficients.reshape(obs * slots, width))


def lane_spread(v, c):
    return jnp.broadcast_to(v[:, c : c + 1], (8, 128))


def inverse_factor(load, put, spare):
    lane = lax.broadcasted_iota(jnp.int32, (8, 128), 1)
    sub = lax.broadcasted_iota(jnp.int32, (8, 128), 0)
    t = [load(g) for g in range(16)]
    for m in range(16):
        s0 = 8 * m
        v = t[m]
        q = m % 2
        for c in range(8):
            spare[q, 8 * c : 8 * c + 8, :] = lane_spread(v, s0 + c)
        inside = (lane >= s0) & (lane < s0 + 8)
        spare[q, 64:72, :] = jnp.where(inside, jnp.where(lane == sub + s0, 1.0, 0.0), v)
        w = [[None] * 8 for _ in range(8)]
        for c in range(8):
            for r in range(c + 1):
                w[r][c] = jnp.broadcast_to(spare[q, 8 * c + r : 8 * c + r + 1, :], (8, 128))
        rows = [jnp.broadcast_to(spare[q, 64 + r : 65 + r, :], (8, 128)) for r in range(8)]
        cols = {g: [lane_spread(t[g], s0 + s) for s in range(8)] for g in range(m + 1, 16)}
        e = None
        recips = []
        for s in range(8):
            pivot = w[s][s]
            recip = 1.0 / pivot
            recips.append(recip)
            es = rows[s] * lax.rsqrt(pivot)
            e = es if e is None else jnp.where(sub >= s, es, e)
            for r in range(8):
                if r == s:
                    continue
                f = (w[s][r] if r > s else w[r][s]) * recip
                for c in range(r if r > s else s + 1, 8):
                    w[r][c] = w[r][c] - f * w[s][c]
                rows[r] = rows[r] - f * rows[s]
        put(m, jnp.where(lane < s0 + 8, e, 0.0))
        y = [rows[s] * recips[s] for s in range(8)]
        for g in range(m + 1, 16):
            acc = [cols[g][s] * y[s] for s in range(8)]
            while len(acc) > 1:
                acc = [acc[i] + acc[i + 1] for i in range(0, len(acc), 2)]
            t[g] = jnp.where(inside, 0.0, t[g]) - acc[0]


def factor_kernel(where_ref, a_ref, factor_ref, solution_ref, a, lh, ll, li, lit, d11, spare, sem):
    copy = pltpu.make_async_copy(a_ref, a, sem)
    copy.start()
    copy.wait()
    low = lax.broadcasted_iota(jnp.int32, (W, W), 0) >= lax.broadcasted_iota(jnp.int32, (W, W), 1)

    def block(idx):
        return pl.ds(pl.multiple_of(idx * W, W), W)

    def step(k, carry):
        d = pl.multiple_of(tri(k, k) * W, W)

        def put0(m, v):
            li[8 * m : 8 * m + 8, 0:128] = v

        def put1(m, v):
            li[128 + 8 * m : 136 + 8 * m, 128:256] = v

        inverse_factor(lambda g: a[pl.ds(d + 8 * g, 8), 0:128], put0, spare)
        li[0:128, 128:256] = jnp.zeros((128, 128), F32)
        i0 = split(li[0:128, 0:128])
        p10 = split(three(nt, split(a[pl.ds(d + 128, 128), 0:128]), i0))
        d11[...] = a[pl.ds(d + 128, 128), 128:256] - three(nt, p10, p10)
        mid = split(three(nn, p10, i0))
        inverse_factor(lambda g: d11[8 * g : 8 * g + 8, :], put1, spare)
        i1 = split(li[128:256, 128:256])
        li[128:256, 0:128] = -three(nn, i1, mid)
        full = li[...]
        lit[k] = full.T
        inv = split(full)

        def panel(i, c):
            rows = block(tri(i, k))
            p = three(nt, split(a[rows, :]), inv)
            p = jnp.where(low | (i > k), p, 0.0)
            a[rows, :] = p
            hi, lo = split(p)
            lh[i] = hi
            ll[i] = lo
            return c

        lax.fori_loop(k, NB, panel, 0)

        def column(j, c):
            bj = (lh[j], ll[j])

            def row(i, c):
                rows = block(tri(i, j))
                a[rows, :] = a[rows, :] - three(nt, (lh[i], ll[i]), (lh[j], ll[j]))
                return c

            return lax.fori_loop(j, NB, row, c)

        lax.fori_loop(k + 1, NB, column, 0)
        return carry

    lax.fori_loop(0, NB, step, 0)

    rhs = a[NP * W : NP * W + NB, :].T
    ys = []
    for k in range(NB):
        w = rhs[:, k : k + 1]
        if k:
            acc = jnp.zeros((W, 128), F32)
            for j in range(k):
                at = tri(k, j) * W
                for h in range(2):
                    acc += a[at : at + W, h * 128 : h * 128 + 128] * ys[j][:, h * 128 : h * 128 + 128]
            w = w - jnp.sum(acc, axis=1, keepdims=True)
        ys.append(jnp.sum(lit[k] * w, axis=0, keepdims=True))
    zs = [None] * NB
    for k in reversed(range(NB)):
        w = ys[k]
        for i in range(k + 1, NB):
            at = tri(i, k) * W
            w = w - jnp.sum(a[at : at + W, :] * zs[i], axis=0, keepdims=True)
        zs[k] = jnp.sum(lit[k] * w, axis=1, keepdims=True)
    lane = lax.broadcasted_iota(jnp.int32, (W, 128), 1)
    z = jnp.zeros((W, 128), F32)
    for k in range(NB):
        z = jnp.where(lane == k, zs[k], z)
    solution_ref[...] = z.T[0:NB, :]

    p = where_ref[0]
    q = where_ref[1]
    for r in range(2):
        for c in range(2):
            i = r * 8 + p
            j = c * 8 + q
            bi = i // 2
            bj = jnp.minimum(j // 2, bi)
            at = pl.multiple_of(tri(bi, bj) * W + (i % 2) * 128, 128)
            both = a[pl.ds(at, 128), :]
            one = jnp.where(j % 2 == 1, both[:, 128:], both[:, :128])
            factor_ref[r, :, c * 128 : c * 128 + 128] = jnp.where(j <= i, one, 0.0)


def factor_and_solve(where, a):
    return pl.pallas_call(
        factor_kernel,
        in_specs=[
            pl.BlockSpec(memory_space=pltpu.SMEM),
            pl.BlockSpec(memory_space=pl.ANY),
        ],
        out_shape=(
            jax.ShapeDtypeStruct((2, BS, 2 * BS), F32),
            jax.ShapeDtypeStruct((NB, W), F32),
        ),
        scratch_shapes=[
            pltpu.VMEM((ROWS, W), F32),
            pltpu.VMEM((NB, W, W), BF16),
            pltpu.VMEM((NB, W, W), BF16),
            pltpu.VMEM((W, W), F32),
            pltpu.VMEM((NB, W, W), F32),
            pltpu.VMEM((128, 128), F32),
            pltpu.VMEM((2, 72, 128), F32),
            pltpu.SemaphoreType.DMA,
        ],
        compiler_params=pltpu.CompilerParams(vmem_limit_bytes=VMEM_LIMIT),
    )(where, a)


def reduce_all(x):
    return lax.psum(x, ALL)


def on_device(blocks, coefficients, residuals):
    where = jnp.stack([lax.axis_index("gx"), lax.axis_index("gy")]).astype(jnp.int32)
    a = reduce_all(gram(blocks, coefficients, residuals))
    factor, answer = factor_and_solve(where, a)
    return factor.reshape(1, 2, BS, 1, 2, BS), answer.reshape(G // BS, BS)


def solution(mesh):
    in_specs = (P(ALL, None), P(ALL, None, None), P(ALL))
    out_specs = (P("gx", None, None, "gy", None, None), P())
    return jax.shard_map(
        on_device, mesh=mesh, in_specs=in_specs, out_specs=out_specs, check_vma=False
    )
```

```python
import jax
import jax.numpy as jnp
from jax import lax
from jax.experimental import pallas as pl
from jax.experimental.pallas import tpu as pltpu
from jax.sharding import PartitionSpec as P

G = 2048
BS = 128
W = 256
NB = G // W
NP = NB * (NB + 1) // 2
CHUNKS = ((0, 2), (2, 8))
SHARES = 64
ALL = ("gx", "gy", "gz")
F32 = jnp.float32
BF16 = jnp.bfloat16
VMEM_LIMIT = 60000 * 1024


def tri(i, j, first=0):
    return (j - first) * NB - (j * (j - 1)) // 2 + (first * (first - 1)) // 2 + (i - j)


def count(first, last):
    return tri(last - 1, last - 1, first) + NB - last + 1


def padded(first, last):
    return 2 * (count(first, last) // 2 + 1)


def share_rows(first, last):
    return padded(first, last) * 2 * BS // SHARES


def nt(a, b):
    return lax.dot_general(a, b, (((1,), (1,)), ((), ())), preferred_element_type=F32)


def nn(a, b):
    return lax.dot_general(a, b, (((1,), (0,)), ((), ())), preferred_element_type=F32)


def split(x):
    hi = x.astype(BF16)
    return hi, (x - hi.astype(F32)).astype(BF16)


def three(dot, a, b):
    return dot(a[0], b[0]) + (dot(a[1], b[0]) + dot(a[0], b[1]))


def gram_kernel(where_ref, meta_ref, other_meta_ref, coef_ref, other_ref, *refs):
    out, c32, ct, marks, dt = refs
    obs = meta_ref.shape[1]
    slots = ct.shape[0]
    scale = 2.0**-17
    core = where_ref[2]
    c32[...] = coef_ref[...].astype(F32)
    parts = []
    for half, (meta, coef) in enumerate(((meta_ref, c32), (other_meta_ref, other_ref))):
        for s in range(slots):
            marks[s, :, pl.ds(half * obs, obs)] = jnp.broadcast_to(
                meta[s : s + 1, :], (16, obs)
            ).astype(BF16)
            for h in range(obs // 128):
                piece = coef[pl.ds(h * 128 * slots + s, 128, stride=slots), :].T
                ct[s, :, pl.ds(half * obs + h * 128, 128)] = piece.astype(BF16)
        r = meta[slots : slots + 1, :]
        r0 = r.astype(BF16).astype(F32)
        r1 = (r - r0).astype(BF16).astype(F32)
        r2 = (r - r0) - r1
        sub = lax.broadcasted_iota(jnp.int32, (8, obs), 0)
        rows = jnp.where(sub == 0, r0, jnp.where(sub == 1, r1, jnp.where(sub == 2, r2, 0.0)))
        parts.append(rows.astype(BF16))
    parts = jnp.concatenate(parts, axis=1)

    def place(b, carry):
        mine = jnp.full((16, 128), b, jnp.int32).astype(F32).astype(BF16)
        for h in range(2 * obs // 128):
            lanes = pl.ds(h * 128, 128)
            picks = [marks[s, :, lanes] == mine for s in range(slots)]
            for g in range(BS // 16):
                d = jnp.zeros((16, 128), BF16)
                for s in range(slots):
                    d = jnp.where(picks[s], ct[s, 16 * g : 16 * g + 16, lanes], d)
                dt[b % 2, b // 2, 16 * g : 16 * g + 16, lanes] = d
        return carry

    lax.fori_loop(0, G // BS, place, 0)

    def put(chunk, idx, rows):
        begin = sum(share_rows(*c) for c in CHUNKS[:chunk])
        size = share_rows(*CHUNKS[chunk])
        at = idx * BS
        done = 0
        while done < rows.shape[0]:
            n = min(rows.shape[0] - done, size - at % size)
            out[at // size, begin + at % size : begin + at % size + n] = rows[done : done + n]
            at += n
            done += n

    for chunk, (first, last) in enumerate(CHUNKS):
        n = count(first, last)
        for idx in range(2 * n, 2 * padded(first, last)):
            put(chunk, idx, jnp.zeros((BS, 128), F32))
    for chunk, (first, last) in enumerate(CHUNKS):
        for j in range(first, last):
            dj = jnp.concatenate([dt[0, j], dt[1, j]], axis=0)
            sums = nt(parts, dj) * scale
            sums = sums[0:1] + (sums[1:2] + sums[2:3])
            size = share_rows(*CHUNKS[0])
            for h in range(2):
                at = (2 * count(*CHUNKS[0]) + h) * BS + j
                out[at // size, at % size : at % size + 1] = sums[:, h * 128 : h * 128 + 128]
            tall = dt[core, j:].reshape((NB - j) * BS, 2 * obs)
            res = nt(tall, dj) * scale
            for i in range(j, NB):
                for h in range(2):
                    rows = res[(i - j) * BS : (i - j) * BS + BS, h * 128 : h * 128 + 128]
                    put(chunk, 2 * tri(i, j, first) + h, rows)


def gram(where, meta, other_meta, coef, other):
    obs = meta.shape[1]
    slots = coef.shape[0] // obs
    return pl.pallas_call(
        gram_kernel,
        in_specs=[pl.BlockSpec(memory_space=pltpu.SMEM)]
        + [pl.BlockSpec(memory_space=pltpu.VMEM)] * 4,
        out_shape=jax.ShapeDtypeStruct(
            (SHARES, sum(share_rows(*c) for c in CHUNKS), 128), F32
        ),
        scratch_shapes=[
            pltpu.VMEM((obs * slots, BS), F32),
            pltpu.VMEM((slots, BS, 2 * obs), BF16),
            pltpu.VMEM((slots, 16, 2 * obs), BF16),
            pltpu.VMEM((2, NB, BS, 2 * obs), BF16),
        ],
        compiler_params=pltpu.CompilerParams(vmem_limit_bytes=VMEM_LIMIT),
        name="gram",
    )(where, meta, other_meta, coef, other)


def lane_spread(v, c):
    return jnp.broadcast_to(v[:, c : c + 1], (8, 128))


def inverse_factor(load, put, spare):
    lane = lax.broadcasted_iota(jnp.int32, (8, 128), 1)
    sub = lax.broadcasted_iota(jnp.int32, (8, 128), 0)
    t = [load(g) for g in range(16)]
    for m in range(16):
        s0 = 8 * m
        v = t[m]
        q = m % 2
        for c in range(8):
            spare[q, 8 * c : 8 * c + 8, :] = lane_spread(v, s0 + c)
        inside = (lane >= s0) & (lane < s0 + 8)
        spare[q, 64:72, :] = jnp.where(inside, jnp.where(lane == sub + s0, 1.0, 0.0), v)
        w = [[None] * 8 for _ in range(8)]
        for c in range(8):
            for r in range(c + 1):
                w[r][c] = jnp.broadcast_to(spare[q, 8 * c + r : 8 * c + r + 1, :], (8, 128))
        rows = [jnp.broadcast_to(spare[q, 64 + r : 65 + r, :], (8, 128)) for r in range(8)]
        cols = {g: [lane_spread(t[g], s0 + s) for s in range(8)] for g in range(m + 1, 16)}
        e = None
        recips = []
        for s in range(8):
            pivot = w[s][s]
            recip = 1.0 / pivot
            recips.append(recip)
            es = rows[s] * lax.rsqrt(pivot)
            e = es if e is None else jnp.where(sub >= s, es, e)
            for r in range(8):
                if r == s:
                    continue
                f = (w[s][r] if r > s else w[r][s]) * recip
                for c in range(r if r > s else s + 1, 8):
                    w[r][c] = w[r][c] - f * w[s][c]
                rows[r] = rows[r] - f * rows[s]
        put(m, jnp.where(lane < s0 + 8, e, 0.0))
        y = [rows[s] * recips[s] for s in range(8)]
        for g in range(m + 1, 16):
            acc = [cols[g][s] * y[s] for s in range(8)]
            while len(acc) > 1:
                acc = [acc[i] + acc[i + 1] for i in range(0, len(acc), 2)]
            t[g] = jnp.where(inside, 0.0, t[g]) - acc[0]


def factor_columns(first, last, a, rhs, lower, lh, ll, li, lit, d11, spare):
    low = lax.broadcasted_iota(jnp.int32, (W, W), 0) >= lax.broadcasted_iota(jnp.int32, (W, W), 1)

    def put_block(idx, v):
        for h in range(2):
            for c in range(2):
                a[idx, c, h] = v[c * 128 : c * 128 + 128, h * 128 : h * 128 + 128]

    def get_block(idx):
        return jnp.concatenate(
            [jnp.concatenate([a[idx, c, 0], a[idx, c, 1]], axis=1) for c in range(2)], axis=0
        )

    def trail(k, begin):
        def column(j, c):
            def row(i, c):
                at = tri(i, j, first)
                put_block(at, get_block(at) - three(nt, (lh[i], ll[i]), (lh[j], ll[j])))
                return c

            return lax.fori_loop(j, NB, row, c)

        lax.fori_loop(begin, last, column, 0)

    def past(k, carry):
        def read(i, c):
            hi, lo = split(lower[tri(i, k)])
            lh[i] = hi
            ll[i] = lo
            return c

        lax.fori_loop(first, NB, read, 0)
        trail(k, first)
        return carry

    if first:
        lax.fori_loop(0, first, past, 0)

    def step(k, carry):
        d = tri(k, k, first)

        def put0(m, v):
            li[8 * m : 8 * m + 8, 0:128] = v

        def put1(m, v):
            li[128 + 8 * m : 136 + 8 * m, 128:256] = v

        inverse_factor(lambda g: a[d, 0, 0, 8 * g : 8 * g + 8, :], put0, spare)
        li[0:128, 128:256] = jnp.zeros((128, 128), F32)
        i0 = split(li[0:128, 0:128])
        p10 = split(three(nt, split(a[d, 1, 0]), i0))
        d11[...] = a[d, 1, 1] - three(nt, p10, p10)
        mid = split(three(nn, p10, i0))
        inverse_factor(lambda g: d11[8 * g : 8 * g + 8, :], put1, spare)
        i1 = split(li[128:256, 128:256])
        li[128:256, 0:128] = -three(nn, i1, mid)
        full = li[...]
        lit[k] = full.T
        inv = split(full)

        def panel(i, c):
            p = three(nt, split(get_block(tri(i, k, first))), inv)
            p = jnp.where(low | (i > k), p, 0.0)
            lower[tri(i, k)] = p
            hi, lo = split(p)
            lh[i] = hi
            ll[i] = lo
            return c

        lax.fori_loop(k, NB, panel, 0)
        trail(k, k + 1)
        return carry

    lax.fori_loop(first, last, step, 0)


def fetch(core, own_ref, other_ref, n, a, sems):
    copies = [
        pltpu.make_async_copy(own_ref.at[pl.ds(0, n)], a.at[:, core], sems.at[0]),
        pltpu.make_async_copy(other_ref.at[pl.ds(0, n)], a.at[:, 1 - core], sems.at[1]),
    ]
    return copies


def first_kernel(where_ref, own_ref, other_ref, lower_ref, lit_ref, a, lh, ll, li, d11, spare, sems):
    first, last = CHUNKS[0]
    copies = fetch(where_ref[2], own_ref, other_ref, count(first, last), a, sems)
    for c in copies:
        c.start()
    for c in copies:
        c.wait()
    factor_columns(first, last, a, None, lower_ref, lh, ll, li, lit_ref, d11, spare)


def last_kernel(
    where_ref, rhs_ref, own_ref, other_ref, lower0_ref, lit0_ref, factor_ref, solution_ref,
    a, lower, lit, lh, ll, li, d11, spare, sems,
):
    first, last = CHUNKS[1]
    n = count(*CHUNKS[0])
    copies = [
        pltpu.make_async_copy(lower0_ref, lower.at[pl.ds(0, n)], sems.at[2]),
        pltpu.make_async_copy(lit0_ref, lit.at[pl.ds(0, first)], sems.at[3]),
    ] + fetch(where_ref[2], own_ref, other_ref, count(first, last), a, sems)
    for c in copies:
        c.start()
    for c in copies:
        c.wait()
    factor_columns(first, last, a, None, lower, lh, ll, li, lit, d11, spare)
    solve(rhs_ref, lower, lit, solution_ref)
    p = where_ref[0]
    q = where_ref[1]
    for r in range(2):
        for c in range(2):
            i = r * 8 + p
            j = c * 8 + q
            bi = i // 2
            bj = jnp.minimum(j // 2, bi)
            both = lower[tri(bi, bj), pl.ds(pl.multiple_of((i % 2) * 128, 128), 128), :]
            one = jnp.where(j % 2 == 1, both[:, 128:], both[:, :128])
            factor_ref[r, :, c * 128 : c * 128 + 128] = jnp.where(j <= i, one, 0.0)


def solve(rhs_ref, lower, lit, solution_ref):
    rhs = rhs_ref[...].T
    ys = []
    for k in range(NB):
        w = jnp.concatenate([rhs[:, k : k + 1], rhs[:, NB + k : NB + k + 1]], axis=0)
        if k:
            acc = jnp.zeros((W, 128), F32)
            for j in range(k):
                for h in range(2):
                    lanes = slice(h * 128, h * 128 + 128)
                    acc += lower[tri(k, j), :, lanes] * ys[j][:, lanes]
            w = w - jnp.sum(acc, axis=1, keepdims=True)
        ys.append(jnp.sum(lit[k] * w, axis=0, keepdims=True))
    zs = [None] * NB
    for k in reversed(range(NB)):
        w = ys[k]
        for i in range(k + 1, NB):
            w = w - jnp.sum(lower[tri(i, k)] * zs[i], axis=0, keepdims=True)
        zs[k] = jnp.sum(lit[k] * w, axis=1, keepdims=True)
    lane = lax.broadcasted_iota(jnp.int32, (W, 128), 1)
    z = jnp.zeros((W, 128), F32)
    for k in range(NB):
        z = jnp.where(lane == k, zs[k], z)
    solution_ref[...] = z.T[0:NB, :]


def work_space(n):
    return [
        pltpu.VMEM((NB, W, W), BF16),
        pltpu.VMEM((NB, W, W), BF16),
        pltpu.VMEM((W, W), F32),
        pltpu.VMEM((128, 128), F32),
        pltpu.VMEM((2, 72, 128), F32),
        pltpu.SemaphoreType.DMA((n,)),
    ]


def blocks_of(n):
    return pltpu.VMEM((n, 2, 2, 128, 128), F32)


def spec(space):
    return pl.BlockSpec(memory_space=space)


def cost(flops):
    return pl.CostEstimate(flops=flops, bytes_accessed=2**23, transcendentals=0)


def factor_first(where, own, other):
    first, last = CHUNKS[0]
    n = count(first, last)
    return pl.pallas_call(
        first_kernel,
        in_specs=[spec(pltpu.SMEM), spec(pl.ANY), spec(pl.ANY)],
        out_shape=(
            jax.ShapeDtypeStruct((n, W, W), F32),
            jax.ShapeDtypeStruct((last, W, W), F32),
        ),
        scratch_shapes=[blocks_of(n)] + work_space(2),
        compiler_params=pltpu.CompilerParams(vmem_limit_bytes=VMEM_LIMIT),
        cost_estimate=cost(10**11),
        name="factor_first",
    )(where, own, other)


def factor_last(where, rhs, own, other, lower, lit):
    return pl.pallas_call(
        last_kernel,
        in_specs=[spec(pltpu.SMEM), spec(pltpu.VMEM)] + [spec(pl.ANY)] * 4,
        out_shape=(
            jax.ShapeDtypeStruct((2, BS, 2 * BS), F32),
            jax.ShapeDtypeStruct((NB, W), F32),
        ),
        scratch_shapes=[
            blocks_of(count(*CHUNKS[1])),
            pltpu.VMEM((NP, W, W), F32),
            pltpu.VMEM((NB, W, W), F32),
        ]
        + work_space(4),
        compiler_params=pltpu.CompilerParams(vmem_limit_bytes=VMEM_LIMIT),
        cost_estimate=cost(10**11),
        name="factor_last",
    )(where, rhs, own, other, lower, lit)


def swap_cores(x):
    size = lax.axis_size("gy")
    return lax.ppermute(x, "gy", [(i, i ^ 1) for i in range(size)])


def exchange(x):
    nx, ny, nz = lax.axis_size("gx"), lax.axis_size("gy"), lax.axis_size("gz")
    groups = [
        [(x * ny + 2 * z + core) * nz + y for x in range(nx) for z in range(ny // 2) for y in range(nz)]
        for core in range(2)
    ]
    return lax.all_to_all(x, ALL, 0, 0, tiled=True, axis_index_groups=groups)


def spread(part):
    return exchange(jnp.broadcast_to(part[None], (SHARES, *part.shape)))


def on_device(blocks, coefficients, residuals):
    obs, slots, width = coefficients.shape
    gy = lax.axis_index("gy")
    where = jnp.stack([lax.axis_index("gx"), gy, gy % 2]).astype(jnp.int32)
    coef = coefficients.reshape(obs * slots, width)
    meta = jnp.concatenate(
        [blocks.T.astype(F32), residuals[None], jnp.zeros((3, obs), F32)], axis=0
    )
    other = swap_cores(coef.astype(F32))
    other_meta = swap_cores(meta)
    sums = gram(where, meta, other_meta, coef, other)
    mine = jnp.sum(exchange(sums), axis=0)
    whole = []
    begin = 0
    for c in CHUNKS:
        rows = share_rows(*c)
        whole.append(spread(mine[begin : begin + rows]).reshape(padded(*c), 2, BS, 128))
        begin += rows
    others = [swap_cores(whole[0])]
    lower, lit = factor_first(where, whole[0], others[0])
    whole[1], lower, lit = lax.optimization_barrier((whole[1], lower, lit))
    others.append(swap_cores(whole[1]))
    n = count(*CHUNKS[0])
    rhs = jnp.where(gy % 2 == 0, whole[0][n, :, 0:NB], others[0][n, :, 0:NB]).reshape(2 * NB, 128)
    factor, answer = factor_last(where, rhs, whole[1], others[1], lower, lit)
    return factor.reshape(1, 2, BS, 1, 2, BS), answer.reshape(G // BS, BS)


def solution(mesh):
    in_specs = (P(ALL, None), P(ALL, None, None), P(ALL))
    out_specs = (P("gx", None, None, "gy", None, None), P())
    return jax.shard_map(
        on_device, mesh=mesh, in_specs=in_specs, out_specs=out_specs, check_vma=False
    )
```

```python
import jax
import jax.numpy as jnp
from jax import lax
from jax.experimental import pallas as pl
from jax.experimental.pallas import tpu as pltpu
from jax.sharding import PartitionSpec as P

G = 2048
BS = 128
W = 256
NB = G // W
NP = NB * (NB + 1) // 2
CHUNKS = ((0, 2), (2, 8))
SHARES = 64
SLOTS = 16
ALL = ("gx", "gy", "gz")
F32 = jnp.float32
BF16 = jnp.bfloat16
VMEM_LIMIT = 60000 * 1024


def tri(i, j, first=0):
    return (j - first) * NB - (j * (j - 1)) // 2 + (first * (first - 1)) // 2 + (i - j)


def count(first, last):
    return tri(last - 1, last - 1, first) + NB - last + 1


def padded(first, last):
    return 2 * (count(first, last) // 2 + 1)


def share_rows(first, last):
    return padded(first, last) * 2 * BS // SHARES


def nt(a, b):
    return lax.dot_general(a, b, (((1,), (1,)), ((), ())), preferred_element_type=F32)


def nn(a, b):
    return lax.dot_general(a, b, (((1,), (0,)), ((), ())), preferred_element_type=F32)


def split(x):
    hi = x.astype(BF16)
    return hi, (x - hi.astype(F32)).astype(BF16)


def three(dot, a, b):
    return dot(a[0], b[0]) + (dot(a[1], b[0]) + dot(a[0], b[1]))


def gram_kernel(where_ref, meta_ref, other_meta_ref, coef_ref, other_ref, *refs):
    out, c32, ct, marks, dt = refs
    obs = meta_ref.shape[1]
    slots = ct.shape[0]
    scale = 2.0**-17
    core = where_ref[2]
    c32[...] = coef_ref[...].astype(F32)
    parts = []
    for half, (meta, coef) in enumerate(((meta_ref, c32), (other_meta_ref, other_ref))):
        for s in range(slots):
            marks[s, :, pl.ds(half * obs, obs)] = jnp.broadcast_to(
                meta[s : s + 1, :], (16, obs)
            ).astype(BF16)
            for h in range(obs // 128):
                piece = coef[pl.ds(h * 128 * slots + s, 128, stride=slots), :].T
                ct[s, :, pl.ds(half * obs + h * 128, 128)] = piece.astype(BF16)
        r = meta[slots : slots + 1, :]
        r0 = r.astype(BF16).astype(F32)
        r1 = (r - r0).astype(BF16).astype(F32)
        r2 = (r - r0) - r1
        sub = lax.broadcasted_iota(jnp.int32, (8, obs), 0)
        rows = jnp.where(sub == 0, r0, jnp.where(sub == 1, r1, jnp.where(sub == 2, r2, 0.0)))
        parts.append(rows.astype(BF16))
    parts = jnp.concatenate(parts, axis=1)

    def place(b, carry):
        mine = jnp.full((16, 128), b, jnp.int32).astype(F32).astype(BF16)
        for h in range(2 * obs // 128):
            lanes = pl.ds(h * 128, 128)
            picks = [marks[s, :, lanes] == mine for s in range(slots)]
            for g in range(BS // 16):
                d = jnp.zeros((16, 128), BF16)
                for s in range(slots):
                    d = jnp.where(picks[s], ct[s, 16 * g : 16 * g + 16, lanes], d)
                dt[b % 2, b // 2, 16 * g : 16 * g + 16, lanes] = d
        return carry

    lax.fori_loop(0, G // BS, place, 0)

    def put(chunk, idx, rows):
        begin = sum(share_rows(*c) for c in CHUNKS[:chunk])
        size = share_rows(*CHUNKS[chunk])
        at = idx * BS
        done = 0
        while done < rows.shape[0]:
            n = min(rows.shape[0] - done, size - at % size)
            out[at // size, begin + at % size : begin + at % size + n] = rows[done : done + n]
            at += n
            done += n

    for chunk, (first, last) in enumerate(CHUNKS):
        n = count(first, last)
        for idx in range(2 * n, 2 * padded(first, last)):
            put(chunk, idx, jnp.zeros((BS, 128), F32))
    for chunk, (first, last) in enumerate(CHUNKS):
        for j in range(first, last):
            dj = jnp.concatenate([dt[0, j], dt[1, j]], axis=0)
            sums = nt(parts, dj) * scale
            sums = sums[0:1] + (sums[1:2] + sums[2:3])
            size = share_rows(*CHUNKS[0])
            for h in range(2):
                at = (2 * count(*CHUNKS[0]) + h) * BS + j
                out[at // size, at % size : at % size + 1] = sums[:, h * 128 : h * 128 + 128]
            tall = dt[core, j:].reshape((NB - j) * BS, 2 * obs)
            res = nt(tall, dj) * scale
            for i in range(j, NB):
                for h in range(2):
                    rows = res[(i - j) * BS : (i - j) * BS + BS, h * 128 : h * 128 + 128]
                    put(chunk, 2 * tri(i, j, first) + h, rows)


def gram(where, meta, other_meta, coef, other):
    obs = meta.shape[1]
    slots = coef.shape[0] // obs
    return pl.pallas_call(
        gram_kernel,
        in_specs=[pl.BlockSpec(memory_space=pltpu.SMEM)]
        + [pl.BlockSpec(memory_space=pltpu.VMEM)] * 4,
        out_shape=jax.ShapeDtypeStruct(
            (SHARES, sum(share_rows(*c) for c in CHUNKS), 128), F32
        ),
        scratch_shapes=[
            pltpu.VMEM((obs * slots, BS), F32),
            pltpu.VMEM((slots, BS, 2 * obs), BF16),
            pltpu.VMEM((slots, 16, 2 * obs), BF16),
            pltpu.VMEM((2, NB, BS, 2 * obs), BF16),
        ],
        compiler_params=pltpu.CompilerParams(vmem_limit_bytes=VMEM_LIMIT),
        name="gram",
    )(where, meta, other_meta, coef, other)


def lane_spread(v, c):
    return jnp.broadcast_to(v[:, c : c + 1], (8, 128))


def inverse_factor(load, put, spare, beside):
    lane = lax.broadcasted_iota(jnp.int32, (8, 128), 1)
    sub = lax.broadcasted_iota(jnp.int32, (8, 128), 0)
    t = [load(g) for g in range(16)]
    for m in range(16):
        s0 = 8 * m
        v = t[m]
        q = m % 2
        for c in range(8):
            spare[q, 8 * c : 8 * c + 8, :] = lane_spread(v, s0 + c)
        inside = (lane >= s0) & (lane < s0 + 8)
        spare[q, 64:72, :] = jnp.where(inside, jnp.where(lane == sub + s0, 1.0, 0.0), v)
        w = [[None] * 8 for _ in range(8)]
        for c in range(8):
            for r in range(c + 1):
                w[r][c] = jnp.broadcast_to(spare[q, 8 * c + r : 8 * c + r + 1, :], (8, 128))
        rows = [jnp.broadcast_to(spare[q, 64 + r : 65 + r, :], (8, 128)) for r in range(8)]
        cols = {g: [lane_spread(t[g], s0 + s) for s in range(8)] for g in range(m + 1, 16)}
        e = None
        recips = []
        for s in range(8):
            pivot = w[s][s]
            recip = 1.0 / pivot
            recips.append(recip)
            es = rows[s] * lax.rsqrt(pivot)
            e = es if e is None else jnp.where(sub >= s, es, e)
            for r in range(8):
                if r == s:
                    continue
                f = (w[s][r] if r > s else w[r][s]) * recip
                for c in range(r if r > s else s + 1, 8):
                    w[r][c] = w[r][c] - f * w[s][c]
                rows[r] = rows[r] - f * rows[s]
        put(m, jnp.where(lane < s0 + 8, e, 0.0))
        if m % 2 == 0:
            beside(m // 2)
        y = [rows[s] * recips[s] for s in range(8)]
        for g in range(m + 1, 16):
            acc = [cols[g][s] * y[s] for s in range(8)]
            while len(acc) > 1:
                acc = [acc[i] + acc[i + 1] for i in range(0, len(acc), 2)]
            t[g] = jnp.where(inside, 0.0, t[g]) - acc[0]


def plan(first, last):
    idle = count(first, last)
    steps = []
    for k in range(NB):
        items = []
        if first <= k < last:
            for m in range(k):
                items += [(tri(i, k, first), tri(i, m), tri(k, m)) for i in range(k + 1, NB)]
                if k + 1 < last:
                    items.append((tri(k + 1, k + 1, first), tri(k + 1, m), tri(k + 1, m)))
        assert len(items) <= SLOTS
        items += [(idle, 0, 0)] * (SLOTS - len(items))
        steps += [t * 4096 + x * 64 + y for t, x, y in items]
    return jnp.array(steps, jnp.int32)


def factor_columns(first, last, plan_ref, a, lower, lh, ll, li, lit, d11, spare):
    low = lax.broadcasted_iota(jnp.int32, (W, W), 0) >= lax.broadcasted_iota(jnp.int32, (W, W), 1)

    def get_block(idx):
        return jnp.concatenate(
            [jnp.concatenate([a[idx, c, 0], a[idx, c, 1]], axis=1) for c in range(2)], axis=0
        )

    def subtract(target, x, y):
        v = three(nt, (lh[x], ll[x]), (lh[y], ll[y]))
        for c in range(2):
            for h in range(2):
                a[target, c, h] = (
                    a[target, c, h] - v[c * 128 : c * 128 + 128, h * 128 : h * 128 + 128]
                )

    def step(k, carry):
        d = tri(k, k, first)

        def beside(n):
            code = plan_ref[k * SLOTS + n]
            subtract(code >> 12, (code >> 6) & 63, code & 63)

        def put0(m, v):
            li[8 * m : 8 * m + 8, 0:128] = v

        def put1(m, v):
            li[128 + 8 * m : 136 + 8 * m, 128:256] = v

        inverse_factor(lambda g: a[d, 0, 0, 8 * g : 8 * g + 8, :], put0, spare, beside)
        li[0:128, 128:256] = jnp.zeros((128, 128), F32)
        i0 = split(li[0:128, 0:128])
        p10 = split(three(nt, split(a[d, 1, 0]), i0))
        d11[...] = a[d, 1, 1] - three(nt, p10, p10)
        mid = split(three(nn, p10, i0))
        inverse_factor(
            lambda g: d11[8 * g : 8 * g + 8, :], put1, spare, lambda n: beside(SLOTS // 2 + n)
        )
        i1 = split(li[128:256, 128:256])
        li[128:256, 0:128] = -three(nn, i1, mid)
        full = li[...]
        lit[k] = full.T
        inv = split(full)

        def panels(t, c):
            for i in (k + 2 * t, jnp.minimum(k + 2 * t + 1, NB - 1)):
                p = three(nt, split(get_block(tri(i, k, first))), inv)
                p = jnp.where(low | (i > k), p, 0.0)
                at = tri(i, k)
                lower[at] = p
                hi, lo = split(p)
                lh[at] = hi
                ll[at] = lo
            return c

        lax.fori_loop(0, (NB - k + 1) // 2, panels, 0)

        @pl.when(k + 1 < last)
        def _():
            at = tri(k + 1, k)
            subtract(tri(k + 1, k + 1, first), at, at)

        return carry

    for m in range(first):
        subtract(tri(first, first, first), tri(first, m), tri(first, m))
    lax.fori_loop(first, last, step, 0)


def fetch(core, own_ref, other_ref, n, a, sems):
    copies = [
        pltpu.make_async_copy(own_ref.at[pl.ds(0, n)], a.at[pl.ds(0, n), core], sems.at[0]),
        pltpu.make_async_copy(other_ref.at[pl.ds(0, n)], a.at[pl.ds(0, n), 1 - core], sems.at[1]),
    ]
    return copies


def first_kernel(
    where_ref, plan_ref, own_ref, other_ref, lower_ref, lh_ref, ll_ref, lit_ref, a, li, d11, spare, sems
):
    first, last = CHUNKS[0]
    copies = fetch(where_ref[2], own_ref, other_ref, count(first, last), a, sems)
    for c in copies:
        c.start()
    for c in copies:
        c.wait()
    factor_columns(first, last, plan_ref, a, lower_ref, lh_ref, ll_ref, li, lit_ref, d11, spare)


def last_kernel(
    where_ref, plan_ref, rhs_ref, own_ref, other_ref, lower0_ref, lh0_ref, ll0_ref, lit0_ref,
    factor_ref, solution_ref, a, li, d11, spare, sems, lower, lit, lh, ll,
):
    first, last = CHUNKS[1]
    n = count(*CHUNKS[0])
    soon = fetch(where_ref[2], own_ref, other_ref, count(first, last), a, sems) + [
        pltpu.make_async_copy(lh0_ref, lh.at[pl.ds(0, n)], sems.at[2]),
        pltpu.make_async_copy(ll0_ref, ll.at[pl.ds(0, n)], sems.at[3]),
    ]
    late = [
        pltpu.make_async_copy(lower0_ref, lower.at[pl.ds(0, n)], sems.at[4]),
        pltpu.make_async_copy(lit0_ref, lit.at[pl.ds(0, first)], sems.at[5]),
    ]
    for c in soon + late:
        c.start()
    for c in soon:
        c.wait()
    factor_columns(first, last, plan_ref, a, lower, lh, ll, li, lit, d11, spare)
    for c in late:
        c.wait()
    solve(rhs_ref, lower, lit, solution_ref)
    p = where_ref[0]
    q = where_ref[1]
    for r in range(2):
        for c in range(2):
            i = r * 8 + p
            j = c * 8 + q
            bi = i // 2
            bj = jnp.minimum(j // 2, bi)
            both = lower[tri(bi, bj), pl.ds(pl.multiple_of((i % 2) * 128, 128), 128), :]
            one = jnp.where(j % 2 == 1, both[:, 128:], both[:, :128])
            factor_ref[r, :, c, :] = jnp.where(j <= i, one, 0.0)


def solve(rhs_ref, lower, lit, solution_ref):
    rhs = rhs_ref[...].T
    ys = []
    for k in range(NB):
        w = jnp.concatenate([rhs[:, k : k + 1], rhs[:, NB + k : NB + k + 1]], axis=0)
        if k:
            acc = jnp.zeros((W, 128), F32)
            for j in range(k):
                for h in range(2):
                    lanes = slice(h * 128, h * 128 + 128)
                    acc += lower[tri(k, j), :, lanes] * ys[j][:, lanes]
            w = w - jnp.sum(acc, axis=1, keepdims=True)
        ys.append(jnp.sum(lit[k] * w, axis=0, keepdims=True))
    lane = lax.broadcasted_iota(jnp.int32, (128, 128), 1)
    z = jnp.zeros((128, 128), F32)
    zs = [None] * NB
    for k in reversed(range(NB)):
        w = ys[k]
        for i in range(k + 1, NB):
            w = w - jnp.sum(lower[tri(i, k)] * zs[i], axis=0, keepdims=True)
        zs[k] = jnp.sum(lit[k] * w, axis=1, keepdims=True)
        z = jnp.where(lane == 2 * k, zs[k][0:128], z)
        z = jnp.where(lane == 2 * k + 1, zs[k][128:256], z)
    solution_ref[...] = z.T[0 : G // BS, :]


def work_space(chunk, n):
    return [
        pltpu.VMEM((count(*chunk) + 1, 2, 2, 128, 128), F32),
        pltpu.VMEM((W, W), F32),
        pltpu.VMEM((128, 128), F32),
        pltpu.VMEM((2, 72, 128), F32),
        pltpu.SemaphoreType.DMA((n,)),
    ]


def spec(space):
    return pl.BlockSpec(memory_space=space)


def cost(flops):
    return pl.CostEstimate(flops=flops, bytes_accessed=2**23, transcendentals=0)


def factor_first(where, own, other):
    first, last = CHUNKS[0]
    n = count(first, last)
    return pl.pallas_call(
        first_kernel,
        in_specs=[spec(pltpu.SMEM), spec(pltpu.SMEM), spec(pl.ANY), spec(pl.ANY)],
        out_shape=(
            jax.ShapeDtypeStruct((n, W, W), F32),
            jax.ShapeDtypeStruct((n, W, W), BF16),
            jax.ShapeDtypeStruct((n, W, W), BF16),
            jax.ShapeDtypeStruct((last, W, W), F32),
        ),
        scratch_shapes=work_space(CHUNKS[0], 2),
        compiler_params=pltpu.CompilerParams(vmem_limit_bytes=VMEM_LIMIT),
        cost_estimate=cost(10**11),
        name="factor_first",
    )(where, plan(first, last), own, other)


def factor_last(where, rhs, own, other, *before):
    return pl.pallas_call(
        last_kernel,
        in_specs=[spec(pltpu.SMEM), spec(pltpu.SMEM), spec(pltpu.VMEM)] + [spec(pl.ANY)] * 6,
        out_shape=(
            jax.ShapeDtypeStruct((2, BS, 2, BS), F32),
            jax.ShapeDtypeStruct((G // BS, BS), F32),
        ),
        scratch_shapes=work_space(CHUNKS[1], 6)
        + [
            pltpu.VMEM((NP, W, W), F32),
            pltpu.VMEM((NB, W, W), F32),
            pltpu.VMEM((NP, W, W), BF16),
            pltpu.VMEM((NP, W, W), BF16),
        ],
        compiler_params=pltpu.CompilerParams(vmem_limit_bytes=VMEM_LIMIT),
        cost_estimate=cost(10**11),
        name="factor_last",
    )(where, plan(*CHUNKS[1]), rhs, own, other, *before)


def swap_cores(x):
    size = lax.axis_size("gy")
    return lax.ppermute(x, "gy", [(i, i ^ 1) for i in range(size)])


def exchange(x):
    nx, ny, nz = lax.axis_size("gx"), lax.axis_size("gy"), lax.axis_size("gz")
    groups = [
        [(x * ny + 2 * z + core) * nz + y for x in range(nx) for z in range(ny // 2) for y in range(nz)]
        for core in range(2)
    ]
    return lax.all_to_all(x, ALL, 0, 0, tiled=True, axis_index_groups=groups)


def spread(part):
    return exchange(jnp.broadcast_to(part[None], (SHARES, *part.shape)))


def on_device(blocks, coefficients, residuals):
    obs, slots, width = coefficients.shape
    gy = lax.axis_index("gy")
    where = jnp.stack([lax.axis_index("gx"), gy, gy % 2]).astype(jnp.int32)
    coef = coefficients.reshape(obs * slots, width)
    meta = jnp.concatenate(
        [blocks.T.astype(F32), residuals[None], jnp.zeros((3, obs), F32)], axis=0
    )
    other = swap_cores(coef.astype(F32))
    other_meta = swap_cores(meta)
    sums = gram(where, meta, other_meta, coef, other)
    mine = jnp.sum(exchange(sums), axis=0)
    whole = []
    begin = 0
    for c in CHUNKS:
        rows = share_rows(*c)
        whole.append(spread(mine[begin : begin + rows]).reshape(padded(*c), 2, BS, 128))
        begin += rows
    others = [swap_cores(whole[0])]
    before = factor_first(where, whole[0], others[0])
    whole[1], *before = lax.optimization_barrier((whole[1], *before))
    others.append(swap_cores(whole[1]))
    n = count(*CHUNKS[0])
    rhs = jnp.where(gy % 2 == 0, whole[0][n, :, 0:NB], others[0][n, :, 0:NB]).reshape(2 * NB, 128)
    factor, answer = factor_last(where, rhs, whole[1], others[1], *before)
    return factor.reshape(1, 2, BS, 1, 2, BS), answer


def solution(mesh):
    in_specs = (P(ALL, None), P(ALL, None, None), P(ALL))
    out_specs = (P("gx", None, None, "gy", None, None), P())
    return jax.shard_map(
        on_device, mesh=mesh, in_specs=in_specs, out_specs=out_specs, check_vma=False
    )
```

```python
import jax
import jax.numpy as jnp
from jax import lax
from jax.experimental import pallas as pl
from jax.experimental.pallas import tpu as pltpu
from jax.sharding import PartitionSpec as P

G = 2048
BS = 128
W = 256
NB = G // W
NP = NB * (NB + 1) // 2
CHUNKS = ((0, 3), (3, 8))
SHARES = 64
SLOTS = 16
ALL = ("gx", "gy", "gz")
F32 = jnp.float32
BF16 = jnp.bfloat16
VMEM_LIMIT = 60000 * 1024


def tri(i, j, first=0):
    return (j - first) * NB - (j * (j - 1)) // 2 + (first * (first - 1)) // 2 + (i - j)


def count(first, last):
    return tri(last - 1, last - 1, first) + NB - last + 1


def padded(first, last):
    return 2 * (count(first, last) // 2 + 1)


def share_rows(first, last):
    return padded(first, last) * 2 * BS // SHARES


def nt(a, b):
    return lax.dot_general(a, b, (((1,), (1,)), ((), ())), preferred_element_type=F32)


def nn(a, b):
    return lax.dot_general(a, b, (((1,), (0,)), ((), ())), preferred_element_type=F32)


def split(x):
    hi = x.astype(BF16)
    return hi, (x - hi.astype(F32)).astype(BF16)


def three(dot, a, b):
    return dot(a[0], b[0]) + (dot(a[1], b[0]) + dot(a[0], b[1]))


def gram_kernel(where_ref, meta_ref, other_meta_ref, coef_ref, other_ref, *refs):
    out, c32, ct, marks, dt = refs
    obs = meta_ref.shape[1]
    slots = ct.shape[0]
    scale = 2.0**-17
    core = where_ref[2]
    c32[...] = coef_ref[...].astype(F32)
    parts = []
    for half, (meta, coef) in enumerate(((meta_ref, c32), (other_meta_ref, other_ref))):
        for s in range(slots):
            marks[s, :, pl.ds(half * obs, obs)] = jnp.broadcast_to(
                meta[s : s + 1, :], (16, obs)
            ).astype(BF16)
            for h in range(obs // 128):
                piece = coef[pl.ds(h * 128 * slots + s, 128, stride=slots), :].astype(BF16)
                ct[s, :, pl.ds(half * obs + h * 128, 128)] = piece.T
        r = meta[slots : slots + 1, :]
        r0 = r.astype(BF16).astype(F32)
        r1 = (r - r0).astype(BF16).astype(F32)
        r2 = (r - r0) - r1
        sub = lax.broadcasted_iota(jnp.int32, (8, obs), 0)
        rows = jnp.where(sub == 0, r0, jnp.where(sub == 1, r1, jnp.where(sub == 2, r2, 0.0)))
        parts.append(rows.astype(BF16))
    parts = jnp.concatenate(parts, axis=1)

    def place(b, carry):
        mine = jnp.full((16, 128), b, jnp.int32).astype(F32).astype(BF16)
        for h in range(2 * obs // 128):
            lanes = pl.ds(h * 128, 128)
            picks = [marks[s, :, lanes] == mine for s in range(slots)]
            for g in range(BS // 16):
                d = jnp.zeros((16, 128), BF16)
                for s in range(slots):
                    d = jnp.where(picks[s], ct[s, 16 * g : 16 * g + 16, lanes], d)
                dt[b % 2, b // 2, 16 * g : 16 * g + 16, lanes] = d
        return carry

    lax.fori_loop(0, G // BS, place, 0)

    def put(chunk, idx, rows):
        begin = sum(share_rows(*c) for c in CHUNKS[:chunk])
        size = share_rows(*CHUNKS[chunk])
        at = idx * BS
        done = 0
        while done < rows.shape[0]:
            n = min(rows.shape[0] - done, size - at % size)
            out[at // size, begin + at % size : begin + at % size + n] = rows[done : done + n]
            at += n
            done += n

    for chunk, (first, last) in enumerate(CHUNKS):
        n = count(first, last)
        for idx in range(2 * n, 2 * padded(first, last)):
            put(chunk, idx, jnp.zeros((BS, 128), F32))
    for chunk, (first, last) in enumerate(CHUNKS):
        for j in range(first, last):
            dj = jnp.concatenate([dt[0, j], dt[1, j]], axis=0)
            sums = nt(parts, dj) * scale
            sums = sums[0:1] + (sums[1:2] + sums[2:3])
            size = share_rows(*CHUNKS[0])
            for h in range(2):
                at = (2 * count(*CHUNKS[0]) + h) * BS + j
                out[at // size, at % size : at % size + 1] = sums[:, h * 128 : h * 128 + 128]
            tall = dt[core, j:].reshape((NB - j) * BS, 2 * obs)
            res = nt(tall, dj) * scale
            for i in range(j, NB):
                for h in range(2):
                    rows = res[(i - j) * BS : (i - j) * BS + BS, h * 128 : h * 128 + 128]
                    put(chunk, 2 * tri(i, j, first) + h, rows)


def gram(where, meta, other_meta, coef, other):
    obs = meta.shape[1]
    slots = coef.shape[0] // obs
    return pl.pallas_call(
        gram_kernel,
        in_specs=[pl.BlockSpec(memory_space=pltpu.SMEM)]
        + [pl.BlockSpec(memory_space=pltpu.VMEM)] * 4,
        out_shape=jax.ShapeDtypeStruct(
            (SHARES, sum(share_rows(*c) for c in CHUNKS), 128), F32
        ),
        scratch_shapes=[
            pltpu.VMEM((obs * slots, BS), F32),
            pltpu.VMEM((slots, BS, 2 * obs), BF16),
            pltpu.VMEM((slots, 16, 2 * obs), BF16),
            pltpu.VMEM((2, NB, BS, 2 * obs), BF16),
        ],
        compiler_params=pltpu.CompilerParams(vmem_limit_bytes=VMEM_LIMIT),
        name="gram",
    )(where, meta, other_meta, coef, other)


def lane_spread(v, c):
    return jnp.broadcast_to(v[:, c : c + 1], (8, 128))


def inverse_factor(load, put, spare, beside):
    lane = lax.broadcasted_iota(jnp.int32, (8, 128), 1)
    sub = lax.broadcasted_iota(jnp.int32, (8, 128), 0)
    t = [load(g) for g in range(16)]
    ahead = [lane_spread(t[0], c) for c in range(8)]
    for m in range(16):
        s0 = 8 * m
        v = t[m]
        q = m % 2
        for c in range(8):
            spare[q, 8 * c : 8 * c + 8, :] = ahead[c]
        inside = (lane >= s0) & (lane < s0 + 8)
        spare[q, 64:72, :] = jnp.where(inside, jnp.where(lane == sub + s0, 1.0, 0.0), v)
        w = [[None] * 8 for _ in range(8)]
        for c in range(8):
            for r in range(c + 1):
                w[r][c] = jnp.broadcast_to(spare[q, 8 * c + r : 8 * c + r + 1, :], (8, 128))
        rows = [jnp.broadcast_to(spare[q, 64 + r : 65 + r, :], (8, 128)) for r in range(8)]
        cols = {g: [lane_spread(t[g], s0 + s) for s in range(8)] for g in range(m + 1, 16)}
        if m < 15:
            near = list(cols[m + 1])
            ahead = [lane_spread(t[m + 1], s0 + 8 + c) for c in range(8)]
        unit = [[None] * 8 for _ in range(8)]
        e = None
        recips = []
        for s in range(8):
            pivot = w[s][s]
            recip = 1.0 / pivot
            recips.append(recip)
            es = rows[s] * lax.rsqrt(pivot)
            e = es if e is None else jnp.where(sub >= s, es, e)
            for r in range(s + 1, 8):
                unit[s][r] = w[s][r] * recip
            for r in range(s + 1, 8):
                for c in range(r, 8):
                    w[r][c] = w[r][c] - unit[s][r] * w[s][c]
                rows[r] = rows[r] - unit[s][r] * rows[s]
                if m < 15:
                    near[r] = near[r] - unit[s][r] * near[s]
            if m < 15:
                at = 72 + 8 * s
                spare[q, at : at + 8, :] = near[s] * recip
                for c in range(8):
                    one = jnp.broadcast_to(spare[q, at + c : at + c + 1, :], (8, 128))
                    ahead[c] = ahead[c] - near[s] * one
        put(m, jnp.where(lane < s0 + 8, e, 0.0))
        if m % 2 == 0:
            beside(m // 2)
        scaled = [rows[s] * recips[s] for s in range(8)]
        y = list(scaled)
        for s in reversed(range(8)):
            for r in range(s):
                y[r] = y[r] - unit[r][s] * y[s]
        for g in range(m + 1, 16):
            left, right = (near, scaled) if g == m + 1 else (cols[g], y)
            acc = [left[s] * right[s] for s in range(8)]
            while len(acc) > 1:
                acc = [acc[i] + acc[i + 1] for i in range(0, len(acc), 2)]
            t[g] = jnp.where(inside, 0.0, t[g]) - acc[0]


def plan(first, last):
    idle = count(first, last)
    steps = []
    for k in range(NB):
        items = []
        if first <= k < last:
            for m in range(k):
                items += [(tri(i, k, first), tri(i, m), tri(k, m)) for i in range(k + 1, NB)]
                if k + 1 < last:
                    items.append((tri(k + 1, k + 1, first), tri(k + 1, m), tri(k + 1, m)))
        assert len(items) <= SLOTS
        items += [(idle, 0, 0)] * (SLOTS - len(items))
        steps += [t * 4096 + x * 64 + y for t, x, y in items]
    return jnp.array(steps, jnp.int32)


def factor_columns(first, last, plan_ref, a, lower, lh, ll, li, lit, d11, spare):
    low = lax.broadcasted_iota(jnp.int32, (W, W), 0) >= lax.broadcasted_iota(jnp.int32, (W, W), 1)

    def get_block(idx):
        return jnp.concatenate(
            [jnp.concatenate([a[idx, c, 0], a[idx, c, 1]], axis=1) for c in range(2)], axis=0
        )

    def subtract(target, x, y):
        v = three(nt, (lh[x], ll[x]), (lh[y], ll[y]))
        for c in range(2):
            for h in range(2):
                a[target, c, h] = (
                    a[target, c, h] - v[c * 128 : c * 128 + 128, h * 128 : h * 128 + 128]
                )

    def step(k, carry):
        d = tri(k, k, first)

        def beside(n):
            code = plan_ref[k * SLOTS + n]
            subtract(code >> 12, (code >> 6) & 63, code & 63)

        def put0(m, v):
            li[8 * m : 8 * m + 8, 0:128] = v

        def put1(m, v):
            li[128 + 8 * m : 136 + 8 * m, 128:256] = v

        inverse_factor(lambda g: a[d, 0, 0, 8 * g : 8 * g + 8, :], put0, spare, beside)
        li[0:128, 128:256] = jnp.zeros((128, 128), F32)
        i0 = split(li[0:128, 0:128])
        p10 = split(three(nt, split(a[d, 1, 0]), i0))
        d11[...] = a[d, 1, 1] - three(nt, p10, p10)
        mid = split(three(nn, p10, i0))
        inverse_factor(
            lambda g: d11[8 * g : 8 * g + 8, :], put1, spare, lambda n: beside(SLOTS // 2 + n)
        )
        i1 = split(li[128:256, 128:256])
        li[128:256, 0:128] = -three(nn, i1, mid)
        full = li[...]
        lit[k] = full.T
        inv = split(full)

        def panels(t, c):
            for i in (k + 2 * t, jnp.minimum(k + 2 * t + 1, NB - 1)):
                p = three(nt, split(get_block(tri(i, k, first))), inv)
                p = jnp.where(low | (i > k), p, 0.0)
                at = tri(i, k)
                lower[at] = p
                hi, lo = split(p)
                lh[at] = hi
                ll[at] = lo
            return c

        lax.fori_loop(0, (NB - k + 1) // 2, panels, 0)

        @pl.when(k + 1 < last)
        def _():
            at = tri(k + 1, k)
            subtract(tri(k + 1, k + 1, first), at, at)

        return carry

    for m in range(first):
        subtract(tri(first, first, first), tri(first, m), tri(first, m))
    lax.fori_loop(first, last, step, 0)


def fetch(core, own_ref, other_ref, n, a, sems):
    copies = [
        pltpu.make_async_copy(own_ref.at[pl.ds(0, n)], a.at[pl.ds(0, n), core], sems.at[0]),
        pltpu.make_async_copy(other_ref.at[pl.ds(0, n)], a.at[pl.ds(0, n), 1 - core], sems.at[1]),
    ]
    return copies


def first_kernel(
    where_ref, plan_ref, own_ref, other_ref, lower_ref, lh_ref, ll_ref, lit_ref, a, li, d11, spare, sems
):
    first, last = CHUNKS[0]
    copies = fetch(where_ref[2], own_ref, other_ref, count(first, last), a, sems)
    for c in copies:
        c.start()
    for c in copies:
        c.wait()
    factor_columns(first, last, plan_ref, a, lower_ref, lh_ref, ll_ref, li, lit_ref, d11, spare)


def last_kernel(
    where_ref, plan_ref, rhs_ref, own_ref, other_ref, lower0_ref, lh0_ref, ll0_ref, lit0_ref,
    factor_ref, solution_ref, a, li, d11, spare, sems, lower, lit, lh, ll,
):
    first, last = CHUNKS[1]
    n = count(*CHUNKS[0])
    soon = fetch(where_ref[2], own_ref, other_ref, count(first, last), a, sems) + [
        pltpu.make_async_copy(lh0_ref, lh.at[pl.ds(0, n)], sems.at[2]),
        pltpu.make_async_copy(ll0_ref, ll.at[pl.ds(0, n)], sems.at[3]),
    ]
    late = [
        pltpu.make_async_copy(lower0_ref, lower.at[pl.ds(0, n)], sems.at[4]),
        pltpu.make_async_copy(lit0_ref, lit.at[pl.ds(0, first)], sems.at[5]),
    ]
    for c in soon + late:
        c.start()
    for c in soon:
        c.wait()
    factor_columns(first, last, plan_ref, a, lower, lh, ll, li, lit, d11, spare)
    for c in late:
        c.wait()
    solve(rhs_ref, lower, lit, solution_ref)
    p = where_ref[0]
    q = where_ref[1]
    for r in range(2):
        for c in range(2):
            i = r * 8 + p
            j = c * 8 + q
            bi = i // 2
            bj = jnp.minimum(j // 2, bi)
            both = lower[tri(bi, bj), pl.ds(pl.multiple_of((i % 2) * 128, 128), 128), :]
            one = jnp.where(j % 2 == 1, both[:, 128:], both[:, :128])
            factor_ref[r, :, c, :] = jnp.where(j <= i, one, 0.0)


def solve(rhs_ref, lower, lit, solution_ref):
    rhs = rhs_ref[...].T
    ys = []
    for k in range(NB):
        w = jnp.concatenate([rhs[:, k : k + 1], rhs[:, NB + k : NB + k + 1]], axis=0)
        if k:
            acc = jnp.zeros((W, 128), F32)
            for j in range(k):
                for h in range(2):
                    lanes = slice(h * 128, h * 128 + 128)
                    acc += lower[tri(k, j), :, lanes] * ys[j][:, lanes]
            w = w - jnp.sum(acc, axis=1, keepdims=True)
        ys.append(jnp.sum(lit[k] * w, axis=0, keepdims=True))
    lane = lax.broadcasted_iota(jnp.int32, (128, 128), 1)
    z = jnp.zeros((128, 128), F32)
    zs = [None] * NB
    for k in reversed(range(NB)):
        w = ys[k]
        for i in range(k + 1, NB):
            w = w - jnp.sum(lower[tri(i, k)] * zs[i], axis=0, keepdims=True)
        zs[k] = jnp.sum(lit[k] * w, axis=1, keepdims=True)
        z = jnp.where(lane == 2 * k, zs[k][0:128], z)
        z = jnp.where(lane == 2 * k + 1, zs[k][128:256], z)
    solution_ref[...] = z.T[0 : G // BS, :]


def work_space(chunk, n):
    return [
        pltpu.VMEM((count(*chunk) + 1, 2, 2, 128, 128), F32),
        pltpu.VMEM((W, W), F32),
        pltpu.VMEM((128, 128), F32),
        pltpu.VMEM((2, 136, 128), F32),
        pltpu.SemaphoreType.DMA((n,)),
    ]


def spec(space):
    return pl.BlockSpec(memory_space=space)


def cost(flops):
    return pl.CostEstimate(flops=flops, bytes_accessed=2**23, transcendentals=0)


def factor_first(where, own, other):
    first, last = CHUNKS[0]
    n = count(first, last)
    return pl.pallas_call(
        first_kernel,
        in_specs=[spec(pltpu.SMEM), spec(pltpu.SMEM), spec(pl.ANY), spec(pl.ANY)],
        out_shape=(
            jax.ShapeDtypeStruct((n, W, W), F32),
            jax.ShapeDtypeStruct((n, W, W), BF16),
            jax.ShapeDtypeStruct((n, W, W), BF16),
            jax.ShapeDtypeStruct((last, W, W), F32),
        ),
        scratch_shapes=work_space(CHUNKS[0], 2),
        compiler_params=pltpu.CompilerParams(vmem_limit_bytes=VMEM_LIMIT),
        cost_estimate=cost(10**11),
        name="factor_first",
    )(where, plan(first, last), own, other)


def factor_last(where, rhs, own, other, *before):
    return pl.pallas_call(
        last_kernel,
        in_specs=[spec(pltpu.SMEM), spec(pltpu.SMEM), spec(pltpu.VMEM)] + [spec(pl.ANY)] * 6,
        out_shape=(
            jax.ShapeDtypeStruct((2, BS, 2, BS), F32),
            jax.ShapeDtypeStruct((G // BS, BS), F32),
        ),
        scratch_shapes=work_space(CHUNKS[1], 6)
        + [
            pltpu.VMEM((NP, W, W), F32),
            pltpu.VMEM((NB, W, W), F32),
            pltpu.VMEM((NP, W, W), BF16),
            pltpu.VMEM((NP, W, W), BF16),
        ],
        compiler_params=pltpu.CompilerParams(vmem_limit_bytes=VMEM_LIMIT),
        cost_estimate=cost(10**11),
        name="factor_last",
    )(where, plan(*CHUNKS[1]), rhs, own, other, *before)


def swap_cores(x):
    size = lax.axis_size("gy")
    return lax.ppermute(x, "gy", [(i, i ^ 1) for i in range(size)])


def exchange(x):
    nx, ny, nz = lax.axis_size("gx"), lax.axis_size("gy"), lax.axis_size("gz")
    groups = [
        [(x * ny + 2 * z + core) * nz + y for x in range(nx) for z in range(ny // 2) for y in range(nz)]
        for core in range(2)
    ]
    return lax.all_to_all(x, ALL, 0, 0, tiled=True, axis_index_groups=groups)


def spread(part):
    return exchange(jnp.broadcast_to(part[None], (SHARES, *part.shape)))


def on_device(blocks, coefficients, residuals):
    obs, slots, width = coefficients.shape
    gy = lax.axis_index("gy")
    where = jnp.stack([lax.axis_index("gx"), gy, gy % 2]).astype(jnp.int32)
    coef = coefficients.reshape(obs * slots, width)
    meta = jnp.concatenate(
        [blocks.T.astype(F32), residuals[None], jnp.zeros((3, obs), F32)], axis=0
    )
    other = swap_cores(coef.astype(F32))
    other_meta = swap_cores(meta)
    sums = gram(where, meta, other_meta, coef, other)
    mine = jnp.sum(exchange(sums), axis=0)
    whole = []
    begin = 0
    for c in CHUNKS:
        rows = share_rows(*c)
        whole.append(spread(mine[begin : begin + rows]).reshape(padded(*c), 2, BS, 128))
        begin += rows
    others = [swap_cores(whole[0])]
    before = factor_first(where, whole[0], others[0])
    whole[1], *before = lax.optimization_barrier((whole[1], *before))
    others.append(swap_cores(whole[1]))
    n = count(*CHUNKS[0])
    rhs = jnp.where(gy % 2 == 0, whole[0][n, :, 0:NB], others[0][n, :, 0:NB]).reshape(2 * NB, 128)
    factor, answer = factor_last(where, rhs, whole[1], others[1], *before)
    return factor.reshape(1, 2, BS, 1, 2, BS), answer


def solution(mesh):
    in_specs = (P(ALL, None), P(ALL, None, None), P(ALL))
    out_specs = (P("gx", None, None, "gy", None, None), P())
    return jax.shard_map(
        on_device, mesh=mesh, in_specs=in_specs, out_specs=out_specs, check_vma=False
    )
```

```python
import jax
import jax.numpy as jnp
from jax import lax
from jax.experimental import pallas as pl
from jax.experimental.pallas import tpu as pltpu
from jax.sharding import PartitionSpec as P

G = 2048
BS = 128
W = 256
NB = G // W
NP = NB * (NB + 1) // 2
CHUNKS = ((0, 3), (3, 8))
SHARES = 64
SLOTS = 16
ALL = ("gx", "gy", "gz")
F32 = jnp.float32
BF16 = jnp.bfloat16
VMEM_LIMIT = 60000 * 1024


def tri(i, j, first=0):
    return (j - first) * NB - (j * (j - 1)) // 2 + (first * (first - 1)) // 2 + (i - j)


def count(first, last):
    return tri(last - 1, last - 1, first) + NB - last + 1


def padded(first, last):
    return 2 * (count(first, last) // 2 + 1)


def share_rows(first, last):
    return padded(first, last) * 2 * BS // SHARES


def nt(a, b):
    return lax.dot_general(a, b, (((1,), (1,)), ((), ())), preferred_element_type=F32)


def nn(a, b):
    return lax.dot_general(a, b, (((1,), (0,)), ((), ())), preferred_element_type=F32)


def split(x):
    hi = x.astype(BF16)
    return hi, (x - hi.astype(F32)).astype(BF16)


def three(dot, a, b):
    return dot(a[0], b[0]) + (dot(a[1], b[0]) + dot(a[0], b[1]))


def gram_kernel(where_ref, meta_ref, other_meta_ref, coef_ref, other_ref, *refs):
    out, c32, ct, marks, dt = refs
    obs = meta_ref.shape[1]
    slots = ct.shape[0]
    scale = 2.0**-17
    core = where_ref[2]
    c32[...] = coef_ref[...].astype(F32)
    parts = []
    for half, (meta, coef) in enumerate(((meta_ref, c32), (other_meta_ref, other_ref))):
        for s in range(slots):
            marks[s, :, pl.ds(half * obs, obs)] = jnp.broadcast_to(
                meta[s : s + 1, :], (16, obs)
            ).astype(BF16)
            for h in range(obs // 128):
                piece = coef[pl.ds(h * 128 * slots + s, 128, stride=slots), :].astype(BF16)
                ct[s, :, pl.ds(half * obs + h * 128, 128)] = piece.T
        r = meta[slots : slots + 1, :]
        r0 = r.astype(BF16).astype(F32)
        r1 = (r - r0).astype(BF16).astype(F32)
        r2 = (r - r0) - r1
        sub = lax.broadcasted_iota(jnp.int32, (8, obs), 0)
        rows = jnp.where(sub == 0, r0, jnp.where(sub == 1, r1, jnp.where(sub == 2, r2, 0.0)))
        parts.append(rows.astype(BF16))
    parts = jnp.concatenate(parts, axis=1)

    def place(b, carry):
        mine = jnp.full((16, 128), b, jnp.int32).astype(F32).astype(BF16)
        for h in range(2 * obs // 128):
            lanes = pl.ds(h * 128, 128)
            picks = [marks[s, :, lanes] == mine for s in range(slots)]
            for g in range(BS // 16):
                d = jnp.zeros((16, 128), BF16)
                for s in range(slots):
                    d = jnp.where(picks[s], ct[s, 16 * g : 16 * g + 16, lanes], d)
                dt[b % 2, b // 2, 16 * g : 16 * g + 16, lanes] = d
        return carry

    lax.fori_loop(0, G // BS, place, 0)

    def put(chunk, idx, rows):
        begin = sum(share_rows(*c) for c in CHUNKS[:chunk])
        size = share_rows(*CHUNKS[chunk])
        at = idx * BS
        done = 0
        while done < rows.shape[0]:
            n = min(rows.shape[0] - done, size - at % size)
            out[at // size, begin + at % size : begin + at % size + n] = rows[done : done + n]
            at += n
            done += n

    for chunk, (first, last) in enumerate(CHUNKS):
        n = count(first, last)
        for idx in range(2 * n, 2 * padded(first, last)):
            put(chunk, idx, jnp.zeros((BS, 128), F32))
    for chunk, (first, last) in enumerate(CHUNKS):
        for j in range(first, last):
            dj = jnp.concatenate([dt[0, j], dt[1, j]], axis=0)
            sums = nt(parts, dj) * scale
            sums = sums[0:1] + (sums[1:2] + sums[2:3])
            size = share_rows(*CHUNKS[0])
            for h in range(2):
                at = (2 * count(*CHUNKS[0]) + h) * BS + j
                out[at // size, at % size : at % size + 1] = sums[:, h * 128 : h * 128 + 128]
            tall = dt[core, j:].reshape((NB - j) * BS, 2 * obs)
            res = nt(tall, dj) * scale
            for i in range(j, NB):
                for h in range(2):
                    rows = res[(i - j) * BS : (i - j) * BS + BS, h * 128 : h * 128 + 128]
                    put(chunk, 2 * tri(i, j, first) + h, rows)


def gram(where, meta, other_meta, coef, other):
    obs = meta.shape[1]
    slots = coef.shape[0] // obs
    return pl.pallas_call(
        gram_kernel,
        in_specs=[pl.BlockSpec(memory_space=pltpu.SMEM)]
        + [pl.BlockSpec(memory_space=pltpu.VMEM)] * 4,
        out_shape=jax.ShapeDtypeStruct(
            (SHARES, sum(share_rows(*c) for c in CHUNKS), 128), F32
        ),
        scratch_shapes=[
            pltpu.VMEM((obs * slots, BS), F32),
            pltpu.VMEM((slots, BS, 2 * obs), BF16),
            pltpu.VMEM((slots, 16, 2 * obs), BF16),
            pltpu.VMEM((2, NB, BS, 2 * obs), BF16),
        ],
        compiler_params=pltpu.CompilerParams(vmem_limit_bytes=VMEM_LIMIT),
        name="gram",
    )(where, meta, other_meta, coef, other)


def lane_spread(v, c):
    return jnp.broadcast_to(v[:, c : c + 1], (8, 128))


REACH = 3


def inverse_factor(load, put, spare, beside):
    lane = lax.broadcasted_iota(jnp.int32, (8, 128), 1)
    sub = lax.broadcasted_iota(jnp.int32, (8, 128), 0)
    t = [load(g) for g in range(16)]
    ahead = [lane_spread(t[0], c) for c in range(8)]
    done = None
    for m in range(16):
        s0 = 8 * m
        q = m % 2
        last = min(m // 2 * 2 + REACH, 15)
        for c in range(8):
            spare[q, 8 * c : 8 * c + 8, :] = ahead[c]
        inside = (lane >= s0) & (lane < s0 + 8)
        spare[q, 64:72, :] = jnp.where(inside, jnp.where(lane == sub + s0, 1.0, 0.0), t[m])
        w = [[None] * 8 for _ in range(8)]
        for c in range(8):
            for r in range(c + 1):
                w[r][c] = jnp.broadcast_to(spare[q, 8 * c + r : 8 * c + r + 1, :], (8, 128))
        rows = [jnp.broadcast_to(spare[q, 64 + r : 65 + r, :], (8, 128)) for r in range(8)]
        cols = {g: [lane_spread(t[g], s0 + s) for s in range(8)] for g in range(m + 1, last + 1)}
        if last < 15 and q == 1:
            back = [lane_spread(done, s0 + s) for s in range(8)]
        if m < 15:
            near = list(cols[m + 1])
            ahead = [lane_spread(t[m + 1], s0 + 8 + c) for c in range(8)]
        unit = [[None] * 8 for _ in range(8)]
        e = None
        recips = []
        for s in range(8):
            pivot = w[s][s]
            recip = 1.0 / pivot
            recips.append(recip)
            es = rows[s] * lax.rsqrt(pivot)
            e = es if e is None else jnp.where(sub >= s, es, e)
            for r in range(s + 1, 8):
                unit[s][r] = w[s][r] * recip
            for r in range(s + 1, 8):
                for c in range(r, 8):
                    w[r][c] = w[r][c] - unit[s][r] * w[s][c]
                rows[r] = rows[r] - unit[s][r] * rows[s]
                if m < 15:
                    near[r] = near[r] - unit[s][r] * near[s]
            if m < 15:
                at = 72 + 8 * s
                spare[q, at : at + 8, :] = near[s] * recip
                for c in range(8):
                    one = jnp.broadcast_to(spare[q, at + c : at + c + 1, :], (8, 128))
                    ahead[c] = ahead[c] - near[s] * one
        put(m, jnp.where(lane < s0 + 8, e, 0.0))
        if m % 2 == 0:
            beside(m // 2)
        scaled = [rows[s] * recips[s] for s in range(8)]
        y = list(scaled)
        for s in reversed(range(8)):
            for r in range(s):
                y[r] = y[r] - unit[r][s] * y[s]

        def less(old, left, right):
            acc = [left[s] * right[s] for s in range(8)]
            while len(acc) > 1:
                acc = [acc[i] + acc[i + 1] for i in range(0, len(acc), 2)]
            return jnp.where(inside, 0.0, old) - acc[0]

        for g in range(m + 1, last + 1):
            t[g] = less(t[g], near, scaled) if g == m + 1 else less(t[g], cols[g], y)
        if last == 15:
            continue
        own = y[0]
        for s in range(1, 8):
            own = jnp.where(sub >= s, y[s], own)
        if q == 0:
            done = own
            continue
        begin = s0 - 8
        full = [jnp.zeros((n, 128), BF16) for n in (begin, 112 - begin) if n]
        reduced = [
            jnp.concatenate(full[: begin > 0] + [x] + full[begin > 0 :], axis=0)
            for x in split(jnp.concatenate([less(done, back, y), own], axis=0))
        ]
        far = jnp.concatenate(t[last + 1 :], axis=0)
        wide = lax.broadcasted_iota(jnp.int32, far.shape, 1)
        kept = jnp.where((wide >= begin) & (wide < begin + 16), 0.0, far)
        far = kept - three(nn, split(far), reduced)
        for g in range(last + 1, 16):
            t[g] = far[8 * (g - last - 1) : 8 * (g - last)]


def plan(first, last):
    idle = count(first, last)
    steps = []
    for k in range(NB):
        items = []
        if first <= k < last:
            for m in range(k):
                items += [(tri(i, k, first), tri(i, m), tri(k, m)) for i in range(k + 1, NB)]
                if k + 1 < last:
                    items.append((tri(k + 1, k + 1, first), tri(k + 1, m), tri(k + 1, m)))
        assert len(items) <= SLOTS
        items += [(idle, 0, 0)] * (SLOTS - len(items))
        steps += [t * 4096 + x * 64 + y for t, x, y in items]
    return jnp.array(steps, jnp.int32)


def factor_columns(first, last, plan_ref, a, lower, lh, ll, li, lit, d11, spare, ready=None):
    low = lax.broadcasted_iota(jnp.int32, (W, W), 0) >= lax.broadcasted_iota(jnp.int32, (W, W), 1)

    def get_block(idx):
        return jnp.concatenate(
            [jnp.concatenate([a[idx, c, 0], a[idx, c, 1]], axis=1) for c in range(2)], axis=0
        )

    def subtract(target, x, y):
        v = three(nt, (lh[x], ll[x]), (lh[y], ll[y]))
        for c in range(2):
            for h in range(2):
                a[target, c, h] = (
                    a[target, c, h] - v[c * 128 : c * 128 + 128, h * 128 : h * 128 + 128]
                )

    def step(k, carry):
        d = tri(k, k, first)

        def beside(n):
            code = plan_ref[k * SLOTS + n]
            subtract(code >> 12, (code >> 6) & 63, code & 63)

        def put0(m, v):
            li[8 * m : 8 * m + 8, 0:128] = v

        def put1(m, v):
            li[128 + 8 * m : 136 + 8 * m, 128:256] = v

        inverse_factor(lambda g: a[d, 0, 0, 8 * g : 8 * g + 8, :], put0, spare, beside)
        li[0:128, 128:256] = jnp.zeros((128, 128), F32)
        i0 = split(li[0:128, 0:128])
        p10 = split(three(nt, split(a[d, 1, 0]), i0))
        d11[...] = a[d, 1, 1] - three(nt, p10, p10)
        mid = split(three(nn, p10, i0))
        inverse_factor(
            lambda g: d11[8 * g : 8 * g + 8, :], put1, spare, lambda n: beside(SLOTS // 2 + n)
        )
        i1 = split(li[128:256, 128:256])
        li[128:256, 0:128] = -three(nn, i1, mid)
        full = li[...]
        lit[k] = full.T
        inv = split(full)

        def panels(t, c):
            for i in (k + 2 * t, jnp.minimum(k + 2 * t + 1, NB - 1)):
                p = three(nt, split(get_block(tri(i, k, first))), inv)
                p = jnp.where(low | (i > k), p, 0.0)
                at = tri(i, k)
                lower[at] = p
                hi, lo = split(p)
                lh[at] = hi
                ll[at] = lo
            return c

        lax.fori_loop(0, (NB - k + 1) // 2, panels, 0)
        if ready is not None:
            ready(k)

        @pl.when(k + 1 < last)
        def _():
            at = tri(k + 1, k)
            subtract(tri(k + 1, k + 1, first), at, at)

        return carry

    for m in range(first):
        subtract(tri(first, first, first), tri(first, m), tri(first, m))
    lax.fori_loop(first, last, step, 0)


def fetch(core, own_ref, other_ref, n, a, sems):
    copies = [
        pltpu.make_async_copy(own_ref.at[pl.ds(0, n)], a.at[pl.ds(0, n), core], sems.at[0]),
        pltpu.make_async_copy(other_ref.at[pl.ds(0, n)], a.at[pl.ds(0, n), 1 - core], sems.at[1]),
    ]
    return copies


def first_kernel(
    where_ref, plan_ref, own_ref, other_ref, lower_ref, lh_ref, ll_ref, lit_ref,
    a, li, d11, spare, sems, lower, lh, ll, out_sems,
):
    first, last = CHUNKS[0]
    copies = fetch(where_ref[2], own_ref, other_ref, count(first, last), a, sems)
    for c in copies:
        c.start()
    for c in copies:
        c.wait()

    def sends(at):
        return [
            pltpu.make_async_copy(x.at[at], y.at[at], out_sems.at[s, at])
            for s, (x, y) in enumerate(((lower, lower_ref), (lh, lh_ref), (ll, ll_ref)))
        ]

    def ready(k):
        def send(i, carry):
            for c in sends(tri(i, k)):
                c.start()
            return carry

        lax.fori_loop(k, NB, send, 0)

    factor_columns(first, last, plan_ref, a, lower, lh, ll, li, lit_ref, d11, spare, ready)

    def finish(at, carry):
        for c in sends(at):
            c.wait()
        return carry

    lax.fori_loop(0, count(first, last), finish, 0)


def last_kernel(
    where_ref, plan_ref, own0_ref, other0_ref, own_ref, other_ref, lower0_ref, lh0_ref, ll0_ref, lit0_ref,
    factor_ref, solution_ref, a, li, d11, spare, sems, lower, lit, lh, ll, rhs,
):
    first, last = CHUNKS[1]
    n = count(*CHUNKS[0])
    soon = fetch(where_ref[2], own_ref, other_ref, count(first, last), a, sems) + [
        pltpu.make_async_copy(lh0_ref, lh.at[pl.ds(0, n)], sems.at[2]),
        pltpu.make_async_copy(ll0_ref, ll.at[pl.ds(0, n)], sems.at[3]),
    ]
    late = [
        pltpu.make_async_copy(lower0_ref, lower.at[pl.ds(0, n)], sems.at[4]),
        pltpu.make_async_copy(lit0_ref, lit.at[pl.ds(0, first)], sems.at[5]),
    ]
    for sem, ref, core in ((6, own0_ref, where_ref[2]), (7, other0_ref, 1 - where_ref[2])):
        rows = ref.at[n, :, pl.ds(0, NB)]
        late.append(pltpu.make_async_copy(rows, rhs.at[core], sems.at[sem]))
    for c in soon + late:
        c.start()
    for c in soon:
        c.wait()
    factor_columns(first, last, plan_ref, a, lower, lh, ll, li, lit, d11, spare)
    for c in late:
        c.wait()
    solve(rhs[0].reshape(2 * NB, 128), lower, lit, solution_ref)
    p = where_ref[0]
    q = where_ref[1]
    for r in range(2):
        for c in range(2):
            i = r * 8 + p
            j = c * 8 + q
            bi = i // 2
            bj = jnp.minimum(j // 2, bi)
            both = lower[tri(bi, bj), pl.ds(pl.multiple_of((i % 2) * 128, 128), 128), :]
            one = jnp.where(j % 2 == 1, both[:, 128:], both[:, :128])
            factor_ref[r, :, c, :] = jnp.where(j <= i, one, 0.0)


def solve(rhs, lower, lit, solution_ref):
    rhs = rhs.T
    ys = []
    for k in range(NB):
        w = jnp.concatenate([rhs[:, k : k + 1], rhs[:, NB + k : NB + k + 1]], axis=0)
        if k:
            acc = jnp.zeros((W, 128), F32)
            for j in range(k):
                for h in range(2):
                    lanes = slice(h * 128, h * 128 + 128)
                    acc += lower[tri(k, j), :, lanes] * ys[j][:, lanes]
            w = w - jnp.sum(acc, axis=1, keepdims=True)
        ys.append(jnp.sum(lit[k] * w, axis=0, keepdims=True))
    lane = lax.broadcasted_iota(jnp.int32, (128, 128), 1)
    z = jnp.zeros((128, 128), F32)
    zs = [None] * NB
    for k in reversed(range(NB)):
        w = ys[k]
        for i in range(k + 1, NB):
            w = w - jnp.sum(lower[tri(i, k)] * zs[i], axis=0, keepdims=True)
        zs[k] = jnp.sum(lit[k] * w, axis=1, keepdims=True)
        z = jnp.where(lane == 2 * k, zs[k][0:128], z)
        z = jnp.where(lane == 2 * k + 1, zs[k][128:256], z)
    solution_ref[...] = z.T[0 : G // BS, :]


def work_space(chunk, n):
    return [
        pltpu.VMEM((count(*chunk) + 1, 2, 2, 128, 128), F32),
        pltpu.VMEM((W, W), F32),
        pltpu.VMEM((128, 128), F32),
        pltpu.VMEM((2, 136, 128), F32),
        pltpu.SemaphoreType.DMA((n,)),
    ]


def spec(space):
    return pl.BlockSpec(memory_space=space)


def cost(flops):
    return pl.CostEstimate(flops=flops, bytes_accessed=2**23, transcendentals=0)


def factor_first(where, own, other):
    first, last = CHUNKS[0]
    n = count(first, last)
    return pl.pallas_call(
        first_kernel,
        in_specs=[spec(pltpu.SMEM), spec(pltpu.SMEM), spec(pl.ANY), spec(pl.ANY)],
        out_shape=(
            jax.ShapeDtypeStruct((n, W, W), F32),
            jax.ShapeDtypeStruct((n, W, W), BF16),
            jax.ShapeDtypeStruct((n, W, W), BF16),
            jax.ShapeDtypeStruct((last, W, W), F32),
        ),
        out_specs=(spec(pl.ANY), spec(pl.ANY), spec(pl.ANY), spec(pltpu.VMEM)),
        scratch_shapes=work_space(CHUNKS[0], 2)
        + [
            pltpu.VMEM((n, W, W), F32),
            pltpu.VMEM((n, W, W), BF16),
            pltpu.VMEM((n, W, W), BF16),
            pltpu.SemaphoreType.DMA((3, n)),
        ],
        compiler_params=pltpu.CompilerParams(vmem_limit_bytes=VMEM_LIMIT),
        cost_estimate=cost(10**11),
        name="factor_first",
    )(where, plan(first, last), own, other)


def factor_last(where, own0, other0, own, other, *before):
    return pl.pallas_call(
        last_kernel,
        in_specs=[spec(pltpu.SMEM)] * 2 + [spec(pl.ANY)] * 8,
        out_shape=(
            jax.ShapeDtypeStruct((2, BS, 2, BS), F32),
            jax.ShapeDtypeStruct((G // BS, BS), F32),
        ),
        scratch_shapes=work_space(CHUNKS[1], 8)
        + [
            pltpu.VMEM((NP, W, W), F32),
            pltpu.VMEM((NB, W, W), F32),
            pltpu.VMEM((NP, W, W), BF16),
            pltpu.VMEM((NP, W, W), BF16),
            pltpu.VMEM((2, 2, NB, 128), F32),
        ],
        compiler_params=pltpu.CompilerParams(vmem_limit_bytes=VMEM_LIMIT),
        cost_estimate=cost(10**11),
        name="factor_last",
    )(where, plan(*CHUNKS[1]), own0, other0, own, other, *before)


def swap_cores(x):
    size = lax.axis_size("gy")
    return lax.ppermute(x, "gy", [(i, i ^ 1) for i in range(size)])


def exchange(x):
    nx, ny, nz = lax.axis_size("gx"), lax.axis_size("gy"), lax.axis_size("gz")
    groups = [
        [(x * ny + 2 * z + core) * nz + y for x in range(nx) for z in range(ny // 2) for y in range(nz)]
        for core in range(2)
    ]
    return lax.all_to_all(x, ALL, 0, 0, tiled=True, axis_index_groups=groups)


def spread(part):
    return exchange(jnp.broadcast_to(part[None], (SHARES, *part.shape)))


def on_device(blocks, coefficients, residuals):
    obs, slots, width = coefficients.shape
    gy = lax.axis_index("gy")
    where = jnp.stack([lax.axis_index("gx"), gy, gy % 2]).astype(jnp.int32)
    coef = coefficients.reshape(obs * slots, width)
    meta = jnp.concatenate(
        [blocks.T.astype(F32), residuals[None], jnp.zeros((3, obs), F32)], axis=0
    )
    other = swap_cores(coef.astype(F32))
    other_meta = swap_cores(meta)
    sums = gram(where, meta, other_meta, coef, other)
    mine = jnp.sum(exchange(sums), axis=0)
    whole = []
    begin = 0
    for c in CHUNKS:
        rows = share_rows(*c)
        whole.append(spread(mine[begin : begin + rows]).reshape(padded(*c), 2, BS, 128))
        begin += rows
    others = [swap_cores(whole[0])]
    before = factor_first(where, whole[0], others[0])
    whole[1], *before = lax.optimization_barrier((whole[1], *before))
    others.append(swap_cores(whole[1]))
    factor, answer = factor_last(where, whole[0], others[0], whole[1], others[1], *before)
    return factor.reshape(1, 2, BS, 1, 2, BS), answer


def solution(mesh):
    in_specs = (P(ALL, None), P(ALL, None, None), P(ALL))
    out_specs = (P("gx", None, None, "gy", None, None), P())
    return jax.shard_map(
        on_device, mesh=mesh, in_specs=in_specs, out_specs=out_specs, check_vma=False
    )
```

```python
import jax
import jax.numpy as jnp
from jax import lax
from jax.experimental import pallas as pl
from jax.experimental.pallas import tpu as pltpu
from jax.sharding import PartitionSpec as P

G = 2048
BS = 128
W = 256
NB = G // W
NP = NB * (NB + 1) // 2
CHUNKS = ((0, 3), (3, 8))
SHARES = 64
SLOTS = 16
ALL = ("gx", "gy", "gz")
F32 = jnp.float32
BF16 = jnp.bfloat16
VMEM_LIMIT = 60000 * 1024


def tri(i, j, first=0):
    return (j - first) * NB - (j * (j - 1)) // 2 + (first * (first - 1)) // 2 + (i - j)


def count(first, last):
    return tri(last - 1, last - 1, first) + NB - last + 1


def padded(first, last):
    return count(first, last) + (1 if first == 0 else -1)


def share_rows(first, last):
    return padded(first, last) * 2 * BS // SHARES


def nt(a, b):
    return lax.dot_general(a, b, (((1,), (1,)), ((), ())), preferred_element_type=F32)


def nn(a, b):
    return lax.dot_general(a, b, (((1,), (0,)), ((), ())), preferred_element_type=F32)


def split(x):
    hi = x.astype(BF16)
    return hi, (x - hi.astype(F32)).astype(BF16)


def three(dot, a, b):
    return dot(a[0], b[0]) + (dot(a[1], b[0]) + dot(a[0], b[1]))


def gram_kernel(where_ref, meta_ref, other_meta_ref, coef_ref, other_ref, *refs):
    out, c32, ct, marks, dt = refs
    obs = meta_ref.shape[1]
    slots = ct.shape[0]
    scale = 2.0**-17
    core = where_ref[2]
    c32[...] = coef_ref[...].astype(F32)
    parts = []
    for half, (meta, coef) in enumerate(((meta_ref, c32), (other_meta_ref, other_ref))):
        for s in range(slots):
            marks[s, :, pl.ds(half * obs, obs)] = jnp.broadcast_to(
                meta[s : s + 1, :], (16, obs)
            ).astype(BF16)
            for h in range(obs // 128):
                piece = coef[pl.ds(h * 128 * slots + s, 128, stride=slots), :].astype(BF16)
                ct[s, :, pl.ds(half * obs + h * 128, 128)] = piece.T
        r = meta[slots : slots + 1, :]
        r0 = r.astype(BF16).astype(F32)
        r1 = (r - r0).astype(BF16).astype(F32)
        r2 = (r - r0) - r1
        sub = lax.broadcasted_iota(jnp.int32, (8, obs), 0)
        rows = jnp.where(sub == 0, r0, jnp.where(sub == 1, r1, jnp.where(sub == 2, r2, 0.0)))
        parts.append(rows.astype(BF16))
    parts = jnp.concatenate(parts, axis=1)

    def place(h, carry):
        lanes = pl.ds(pl.multiple_of(h * 128, 128), 128)
        kept = [[ct[s, 16 * g : 16 * g + 16, lanes] for g in range(BS // 16)] for s in range(slots)]
        named = [marks[s, :, lanes] for s in range(slots)]
        for b in range(G // BS):
            picks = [m == jnp.full((16, 128), b, BF16) for m in named]
            for g in range(BS // 16):
                d = jnp.zeros((16, 128), BF16)
                for s in range(slots):
                    d = jnp.where(picks[s], kept[s][g], d)
                dt[b % 2, b // 2, 16 * g : 16 * g + 16, lanes] = d
        return carry

    lax.fori_loop(0, 2 * obs // 128, place, 0)

    def put(chunk, idx, rows):
        begin = sum(share_rows(*c) for c in CHUNKS[:chunk])
        size = share_rows(*CHUNKS[chunk])
        at = idx * BS
        done = 0
        while done < rows.shape[0]:
            n = min(rows.shape[0] - done, size - at % size)
            out[at // size, begin + at % size : begin + at % size + n] = rows[done : done + n]
            at += n
            done += n

    sums = []
    for chunk, (first, last) in enumerate(CHUNKS):
        for j in range(first, last):
            dj = jnp.concatenate([dt[0, j], dt[1, j]], axis=0)
            one = nt(parts, dj) * scale
            sums.append(one[0:1] + (one[1:2] + one[2:3]))
            tall = dt[core, j:].reshape((NB - j) * BS, 2 * obs)
            res = nt(tall, dj) * scale
            for i in range(j, NB):
                for h in range(2):
                    rows = res[(i - j) * BS : (i - j) * BS + BS, h * 128 : h * 128 + 128]
                    if j == NB - 1:
                        put(0, 2 * count(*CHUNKS[0]) + h, rows)
                    else:
                        put(chunk, 2 * tri(i, j, first) + h, rows)
    size = share_rows(*CHUNKS[0])
    for j in range(NB):
        for h in range(2):
            at = BS + h * NB + j
            here = pl.ds(at % size, 1)
            one = sums[j][:, h * 128 : h * 128 + 128]
            out[at // size, here] = jnp.where(core == 0, one, out[at // size, here])


def gram(where, meta, other_meta, coef, other):
    obs = meta.shape[1]
    slots = coef.shape[0] // obs
    return pl.pallas_call(
        gram_kernel,
        in_specs=[pl.BlockSpec(memory_space=pltpu.SMEM)]
        + [pl.BlockSpec(memory_space=pltpu.VMEM)] * 4,
        out_shape=jax.ShapeDtypeStruct(
            (SHARES, sum(share_rows(*c) for c in CHUNKS), 128), F32
        ),
        scratch_shapes=[
            pltpu.VMEM((obs * slots, BS), F32),
            pltpu.VMEM((slots, BS, 2 * obs), BF16),
            pltpu.VMEM((slots, 16, 2 * obs), BF16),
            pltpu.VMEM((2, NB, BS, 2 * obs), BF16),
        ],
        compiler_params=pltpu.CompilerParams(vmem_limit_bytes=VMEM_LIMIT),
        name="gram",
    )(where, meta, other_meta, coef, other)


def lane_spread(v, c):
    return jnp.broadcast_to(v[:, c : c + 1], (8, 128))


REACH = 3


def inverse_factor(load, put, spare, beside):
    lane = lax.broadcasted_iota(jnp.int32, (8, 128), 1)
    sub = lax.broadcasted_iota(jnp.int32, (8, 128), 0)
    t = [load(g) for g in range(16)]
    ahead = [lane_spread(t[0], c) for c in range(8)]
    done = None
    for m in range(16):
        s0 = 8 * m
        q = m % 2
        last = min(m // 2 * 2 + REACH, 15)
        for c in range(8):
            spare[q, 8 * c : 8 * c + 8, :] = ahead[c]
        inside = (lane >= s0) & (lane < s0 + 8)
        spare[q, 64:72, :] = jnp.where(inside, jnp.where(lane == sub + s0, 1.0, 0.0), t[m])
        w = [[None] * 8 for _ in range(8)]
        for c in range(8):
            for r in range(c + 1):
                w[r][c] = jnp.broadcast_to(spare[q, 8 * c + r : 8 * c + r + 1, :], (8, 128))
        rows = [jnp.broadcast_to(spare[q, 64 + r : 65 + r, :], (8, 128)) for r in range(8)]
        cols = {g: [lane_spread(t[g], s0 + s) for s in range(8)] for g in range(m + 1, last + 1)}
        if last < 15 and q == 1:
            back = [lane_spread(done, s0 + s) for s in range(8)]
        if m < 15:
            near = list(cols[m + 1])
            ahead = [lane_spread(t[m + 1], s0 + 8 + c) for c in range(8)]
        unit = [[None] * 8 for _ in range(8)]
        e = None
        recips = []
        for s in range(8):
            pivot = w[s][s]
            recip = 1.0 / pivot
            recips.append(recip)
            es = rows[s] * lax.rsqrt(pivot)
            e = es if e is None else jnp.where(sub >= s, es, e)
            for r in range(s + 1, 8):
                unit[s][r] = w[s][r] * recip
            for r in range(s + 1, 8):
                for c in range(r, 8):
                    w[r][c] = w[r][c] - unit[s][r] * w[s][c]
                rows[r] = rows[r] - unit[s][r] * rows[s]
                if m < 15:
                    near[r] = near[r] - unit[s][r] * near[s]
            if m < 15:
                at = 72 + 8 * s
                spare[q, at : at + 8, :] = near[s] * recip
                for c in range(8):
                    one = jnp.broadcast_to(spare[q, at + c : at + c + 1, :], (8, 128))
                    ahead[c] = ahead[c] - near[s] * one
        put(m, jnp.where(lane < s0 + 8, e, 0.0))
        if m % 2 == 0:
            beside(m // 2)
        scaled = [rows[s] * recips[s] for s in range(8)]
        y = list(scaled)
        for s in reversed(range(8)):
            for r in range(s):
                y[r] = y[r] - unit[r][s] * y[s]

        def less(old, left, right):
            acc = [left[s] * right[s] for s in range(8)]
            while len(acc) > 1:
                acc = [acc[i] + acc[i + 1] for i in range(0, len(acc), 2)]
            return jnp.where(inside, 0.0, old) - acc[0]

        for g in range(m + 1, last + 1):
            t[g] = less(t[g], near, scaled) if g == m + 1 else less(t[g], cols[g], y)
        if last == 15:
            continue
        own = y[0]
        for s in range(1, 8):
            own = jnp.where(sub >= s, y[s], own)
        if q == 0:
            done = own
            continue
        begin = s0 - 8
        full = [jnp.zeros((n, 128), BF16) for n in (begin, 112 - begin) if n]
        reduced = [
            jnp.concatenate(full[: begin > 0] + [x] + full[begin > 0 :], axis=0)
            for x in split(jnp.concatenate([less(done, back, y), own], axis=0))
        ]
        far = jnp.concatenate(t[last + 1 :], axis=0)
        wide = lax.broadcasted_iota(jnp.int32, far.shape, 1)
        kept = jnp.where((wide >= begin) & (wide < begin + 16), 0.0, far)
        far = kept - three(nn, split(far), reduced)
        for g in range(last + 1, 16):
            t[g] = far[8 * (g - last - 1) : 8 * (g - last)]


def plan(first, last):
    idle = count(first, last)
    steps = []
    for k in range(NB):
        items = []
        if first <= k < last:
            for m in range(k):
                items += [(tri(i, k, first), tri(i, m), tri(k, m)) for i in range(k + 1, NB)]
                if k + 1 < last:
                    items.append((tri(k + 1, k + 1, first), tri(k + 1, m), tri(k + 1, m)))
        assert len(items) <= SLOTS
        items += [(idle, 0, 0)] * (SLOTS - len(items))
        steps += [t * 4096 + x * 64 + y for t, x, y in items]
    return jnp.array(steps, jnp.int32)


def factor_columns(first, last, plan_ref, a, lower, lh, ll, li, lit, d11, spare, ready=None):
    low = lax.broadcasted_iota(jnp.int32, (W, W), 0) >= lax.broadcasted_iota(jnp.int32, (W, W), 1)

    def get_block(idx):
        return jnp.concatenate(
            [jnp.concatenate([a[idx, c, 0], a[idx, c, 1]], axis=1) for c in range(2)], axis=0
        )

    def subtract(target, x, y):
        v = three(nt, (lh[x], ll[x]), (lh[y], ll[y]))
        for c in range(2):
            for h in range(2):
                a[target, c, h] = (
                    a[target, c, h] - v[c * 128 : c * 128 + 128, h * 128 : h * 128 + 128]
                )

    def step(k, carry):
        d = tri(k, k, first)

        def beside(n):
            code = plan_ref[k * SLOTS + n]
            subtract(code >> 12, (code >> 6) & 63, code & 63)

        def put0(m, v):
            li[8 * m : 8 * m + 8, 0:128] = v

        def put1(m, v):
            li[128 + 8 * m : 136 + 8 * m, 128:256] = v

        inverse_factor(lambda g: a[d, 0, 0, 8 * g : 8 * g + 8, :], put0, spare, beside)
        li[0:128, 128:256] = jnp.zeros((128, 128), F32)
        i0 = split(li[0:128, 0:128])
        p10 = split(three(nt, split(a[d, 1, 0]), i0))
        d11[...] = a[d, 1, 1] - three(nt, p10, p10)
        mid = split(three(nn, p10, i0))
        inverse_factor(
            lambda g: d11[8 * g : 8 * g + 8, :], put1, spare, lambda n: beside(SLOTS // 2 + n)
        )
        i1 = split(li[128:256, 128:256])
        li[128:256, 0:128] = -three(nn, i1, mid)
        full = li[...]
        lit[k] = full.T
        inv = split(full)

        def panels(t, c):
            for i in (k + 2 * t, jnp.minimum(k + 2 * t + 1, NB - 1)):
                p = three(nt, split(get_block(tri(i, k, first))), inv)
                p = jnp.where(low | (i > k), p, 0.0)
                at = tri(i, k)
                lower[at] = p
                hi, lo = split(p)
                lh[at] = hi
                ll[at] = lo
            return c

        lax.fori_loop(0, (NB - k + 1) // 2, panels, 0)
        if ready is not None:
            ready(k)

        @pl.when(k + 1 < last)
        def _():
            at = tri(k + 1, k)
            subtract(tri(k + 1, k + 1, first), at, at)

        return carry

    for m in range(first):
        subtract(tri(first, first, first), tri(first, m), tri(first, m))
    lax.fori_loop(first, last, step, 0)


def fetch(core, own_ref, other_ref, n, a, sems):
    copies = [
        pltpu.make_async_copy(own_ref.at[pl.ds(0, n)], a.at[pl.ds(0, n), core], sems.at[0]),
        pltpu.make_async_copy(other_ref.at[pl.ds(0, n)], a.at[pl.ds(0, n), 1 - core], sems.at[1]),
    ]
    return copies


def first_kernel(
    where_ref, plan_ref, own_ref, other_ref, lower_ref, lh_ref, ll_ref, lit_ref,
    a, li, d11, spare, sems, lower, lh, ll, out_sems,
):
    first, last = CHUNKS[0]
    copies = fetch(where_ref[2], own_ref, other_ref, count(first, last), a, sems)
    for c in copies:
        c.start()
    for c in copies:
        c.wait()

    def sends(at):
        return [
            pltpu.make_async_copy(x.at[at], y.at[at], out_sems.at[s, at])
            for s, (x, y) in enumerate(((lower, lower_ref), (lh, lh_ref), (ll, ll_ref)))
        ]

    def ready(k):
        def send(i, carry):
            for c in sends(tri(i, k)):
                c.start()
            return carry

        lax.fori_loop(k, NB, send, 0)

    factor_columns(first, last, plan_ref, a, lower, lh, ll, li, lit_ref, d11, spare, ready)

    def finish(at, carry):
        for c in sends(at):
            c.wait()
        return carry

    lax.fori_loop(0, count(first, last), finish, 0)


def last_kernel(
    where_ref, plan_ref, own0_ref, other0_ref, own_ref, other_ref, lower0_ref, lh0_ref, ll0_ref, lit0_ref,
    factor_ref, solution_ref, a, li, d11, spare, sems, lower, lit, lh, ll, rhs,
):
    first, last = CHUNKS[1]
    n = count(*CHUNKS[0])
    m = padded(first, last)
    core = where_ref[2]
    soon = fetch(core, own_ref, other_ref, m, a, sems) + [
        pltpu.make_async_copy(own0_ref.at[n], a.at[m, core], sems.at[8]),
        pltpu.make_async_copy(other0_ref.at[n], a.at[m, 1 - core], sems.at[9]),
        pltpu.make_async_copy(lh0_ref, lh.at[pl.ds(0, n)], sems.at[2]),
        pltpu.make_async_copy(ll0_ref, ll.at[pl.ds(0, n)], sems.at[3]),
    ]
    late = [
        pltpu.make_async_copy(lower0_ref, lower.at[pl.ds(0, n)], sems.at[4]),
        pltpu.make_async_copy(lit0_ref, lit.at[pl.ds(0, first)], sems.at[5]),
    ]
    for sem, ref, side in ((6, own0_ref, core), (7, other0_ref, 1 - core)):
        rows = ref.at[0, 1, pl.ds(0, 2 * NB)]
        late.append(pltpu.make_async_copy(rows, rhs.at[side], sems.at[sem]))
    for c in soon + late:
        c.start()
    for c in soon:
        c.wait()
    factor_columns(first, last, plan_ref, a, lower, lh, ll, li, lit, d11, spare)
    for c in late:
        c.wait()
    solve(rhs[0], lower, lit, solution_ref)
    p = where_ref[0]
    q = where_ref[1]
    for r in range(2):
        for c in range(2):
            i = r * 8 + p
            j = c * 8 + q
            bi = i // 2
            bj = jnp.minimum(j // 2, bi)
            both = lower[tri(bi, bj), pl.ds(pl.multiple_of((i % 2) * 128, 128), 128), :]
            one = jnp.where(j % 2 == 1, both[:, 128:], both[:, :128])
            factor_ref[r, :, c, :] = jnp.where(j <= i, one, 0.0)


def solve(rhs, lower, lit, solution_ref):
    rhs = rhs.T
    ys = []
    for k in range(NB):
        w = jnp.concatenate([rhs[:, k : k + 1], rhs[:, NB + k : NB + k + 1]], axis=0)
        if k:
            acc = jnp.zeros((W, 128), F32)
            for j in range(k):
                for h in range(2):
                    lanes = slice(h * 128, h * 128 + 128)
                    acc += lower[tri(k, j), :, lanes] * ys[j][:, lanes]
            w = w - jnp.sum(acc, axis=1, keepdims=True)
        ys.append(jnp.sum(lit[k] * w, axis=0, keepdims=True))
    lane = lax.broadcasted_iota(jnp.int32, (128, 128), 1)
    z = jnp.zeros((128, 128), F32)
    zs = [None] * NB
    for k in reversed(range(NB)):
        w = ys[k]
        for i in range(k + 1, NB):
            w = w - jnp.sum(lower[tri(i, k)] * zs[i], axis=0, keepdims=True)
        zs[k] = jnp.sum(lit[k] * w, axis=1, keepdims=True)
        z = jnp.where(lane == 2 * k, zs[k][0:128], z)
        z = jnp.where(lane == 2 * k + 1, zs[k][128:256], z)
    solution_ref[...] = z.T[0 : G // BS, :]


def work_space(chunk, n):
    return [
        pltpu.VMEM((count(*chunk) + 1, 2, 2, 128, 128), F32),
        pltpu.VMEM((W, W), F32),
        pltpu.VMEM((128, 128), F32),
        pltpu.VMEM((2, 136, 128), F32),
        pltpu.SemaphoreType.DMA((n,)),
    ]


def spec(space):
    return pl.BlockSpec(memory_space=space)


def cost(flops):
    return pl.CostEstimate(flops=flops, bytes_accessed=2**23, transcendentals=0)


def factor_first(where, own, other):
    first, last = CHUNKS[0]
    n = count(first, last)
    return pl.pallas_call(
        first_kernel,
        in_specs=[spec(pltpu.SMEM), spec(pltpu.SMEM), spec(pl.ANY), spec(pl.ANY)],
        out_shape=(
            jax.ShapeDtypeStruct((n, W, W), F32),
            jax.ShapeDtypeStruct((n, W, W), BF16),
            jax.ShapeDtypeStruct((n, W, W), BF16),
            jax.ShapeDtypeStruct((last, W, W), F32),
        ),
        out_specs=(spec(pl.ANY), spec(pl.ANY), spec(pl.ANY), spec(pltpu.VMEM)),
        scratch_shapes=work_space(CHUNKS[0], 2)
        + [
            pltpu.VMEM((n, W, W), F32),
            pltpu.VMEM((n, W, W), BF16),
            pltpu.VMEM((n, W, W), BF16),
            pltpu.SemaphoreType.DMA((3, n)),
        ],
        compiler_params=pltpu.CompilerParams(vmem_limit_bytes=VMEM_LIMIT),
        cost_estimate=cost(10**11),
        name="factor_first",
    )(where, plan(first, last), own, other)


def factor_last(where, own0, other0, own, other, *before):
    return pl.pallas_call(
        last_kernel,
        in_specs=[spec(pltpu.SMEM)] * 2 + [spec(pl.ANY)] * 8,
        out_shape=(
            jax.ShapeDtypeStruct((2, BS, 2, BS), F32),
            jax.ShapeDtypeStruct((G // BS, BS), F32),
        ),
        scratch_shapes=work_space(CHUNKS[1], 10)
        + [
            pltpu.VMEM((NP, W, W), F32),
            pltpu.VMEM((NB, W, W), F32),
            pltpu.VMEM((NP, W, W), BF16),
            pltpu.VMEM((NP, W, W), BF16),
            pltpu.VMEM((2, 2 * NB, 128), F32),
        ],
        compiler_params=pltpu.CompilerParams(vmem_limit_bytes=VMEM_LIMIT),
        cost_estimate=cost(10**11),
        name="factor_last",
    )(where, plan(*CHUNKS[1]), own0, other0, own, other, *before)


def swap_cores(x):
    size = lax.axis_size("gy")
    return lax.ppermute(x, "gy", [(i, i ^ 1) for i in range(size)])


def exchange(x):
    nx, ny, nz = lax.axis_size("gx"), lax.axis_size("gy"), lax.axis_size("gz")
    groups = [
        [(x * ny + 2 * z + core) * nz + y for x in range(nx) for z in range(ny // 2) for y in range(nz)]
        for core in range(2)
    ]
    return lax.all_to_all(x, ALL, 0, 0, tiled=True, axis_index_groups=groups)


def on_device(blocks, coefficients, residuals):
    obs, slots, width = coefficients.shape
    gy = lax.axis_index("gy")
    where = jnp.stack([lax.axis_index("gx"), gy, gy % 2]).astype(jnp.int32)
    coef = coefficients.reshape(obs * slots, width)
    meta = jnp.concatenate(
        [blocks.T.astype(F32), residuals[None], jnp.zeros((3, obs), F32)], axis=0
    )
    other = swap_cores(coef.astype(F32))
    other_meta = swap_cores(meta)
    sums = gram(where, meta, other_meta, coef, other)
    mine = jnp.sum(exchange(sums), axis=0)
    split_at = share_rows(*CHUNKS[0])
    again = [jnp.broadcast_to(x[None], (SHARES, *x.shape)) for x in (mine[:split_at], mine[split_at:])]
    whole = [exchange(again[0]), None]
    whole[0], again[1] = lax.optimization_barrier((whole[0], again[1]))
    whole[1] = exchange(again[1])
    whole = [x.reshape(padded(*c), 2, BS, 128) for x, c in zip(whole, CHUNKS)]
    others = [swap_cores(whole[0])]
    before = factor_first(where, whole[0], others[0])
    whole[1], *before = lax.optimization_barrier((whole[1], *before))
    others.append(swap_cores(whole[1]))
    factor, answer = factor_last(where, whole[0], others[0], whole[1], others[1], *before)
    return factor.reshape(1, 2, BS, 1, 2, BS), answer


def solution(mesh):
    in_specs = (P(ALL, None), P(ALL, None, None), P(ALL))
    out_specs = (P("gx", None, None, "gy", None, None), P())
    return jax.shard_map(
        on_device, mesh=mesh, in_specs=in_specs, out_specs=out_specs, check_vma=False
    )
```
